256 devices in a mesh: groups: 2 (over y), seq: 16 (over z), section: 4 (over x), mp: 2 (over core).
Axes of the slice: x: 4, y: 2, z: 16, core: 2. Of those that a mesh axis runs over, the one named last changes fastest.
The devices are a block of a 4x16x16 slice.
Arguments:
- light_queries: bfloat16 [8192, 8192], P(('groups', 'seq'), ('section', 'mp')), parts along dimension 0, may hold values from -6 to 6
- light_keys: bfloat16 [8192, 8192], P(('groups', 'seq'), ('section', 'mp')), parts along dimension 0, may hold values from -6 to 6
- light_values: bfloat16 [8192, 8192], P(('groups', 'seq'), ('section', 'mp')), parts along dimension 0, may hold values from -6 to 6
- decay_log: float32 [8192, 64], P(('groups', 'seq'), ('section', 'mp')), parts along dimension 0, may hold values from -1 to 0
- norm_gain: float32 [8192], P(('section', 'mp')), may hold values from 0.25 to 1.75
- soft_queries: bfloat16 [8192, 8192], P(('groups', 'seq'), ('section', 'mp')), parts along dimension 0, may hold values from -150 to 150
- soft_keys: bfloat16 [8192, 1024], P(('groups', 'seq'), ('section', 'mp')), parts along dimension 0, may hold values from -6 to 6
- soft_values: bfloat16 [8192, 1024], P(('groups', 'seq'), ('section', 'mp')), parts along dimension 0, may hold values from -6 to 6
- lengths: int32 [32], P('groups'), parts along dimension 0, may hold values from 1 to 256, 3072 in all
Outputs:
- light_out: bfloat16 [8192, 8192], P(('groups', 'seq'), ('section', 'mp')), parts along dimension 0
- soft_out: bfloat16 [8192, 8192], P(('groups', 'seq'), ('section', 'mp')), parts along dimension 0
The draws below stay inside these ranges and needn't reach their ends.
There are 2 independent parts, one for each index of `groups`. The reference program is written for one: setup_inputs(seed, part) draws one part's arguments, and reference() takes and returns one part's arrays. A program takes and returns all parts, laid end to end along the dimension named above; an argument that names none is the same for every part. Nothing has to cross between parts.
Inputs may be any that keep to these rules, and one draw needn't show every extreme that they name: The live tokens of a block stand at its first slots; the lengths sum to 3072.
All inputs are finite; a program needn't handle non-finite values.
Results may differ from the reference program's by a relative error of at most 0.007.
Values may be sent and summed in bfloat16 or wider, within the bound.
No kernel may reach another device: no remote copies, remote signals or barrier semaphores. Data moves between devices by JAX's collectives and lax.ppermute only.
A program may use at most 64 MiB of HBM per device.

```python
import math
import jax
import jax.numpy as jnp
import numpy as np
from jax import lax

QUERY_HEAD_COUNT = 64
KV_HEADS = 8
HEAD_DIM = 128
TOK_DEV = 256
TOKEN_SLOTS = 4096
N_SEQ = 16


def draw_decay_log(key, part):
    random_subkeys = jax.random.split(jax.random.fold_in(key, 3), 8)
    slow_share = 0.5
    slow_heads = jax.random.uniform(random_subkeys[0], (QUERY_HEAD_COUNT,)) < slow_share
    slow_rate = jax.random.uniform(random_subkeys[1], (QUERY_HEAD_COUNT,), minval=0.05, maxval=0.2) * math.log(10.0) / TOKEN_SLOTS
    fast_rate = 1.0 / jax.random.uniform(random_subkeys[2], (QUERY_HEAD_COUNT,), minval=30.0, maxval=50.0)
    head_decay_rate = jnp.where(slow_heads, slow_rate, fast_rate)
    block_count = TOKEN_SLOTS // TOK_DEV
    block_multiplier = jnp.repeat(jax.random.uniform(random_subkeys[3], (block_count, QUERY_HEAD_COUNT), minval=0.6, maxval=1.4), TOK_DEV, axis=0)
    slot_multiplier = jax.random.uniform(random_subkeys[4], (TOKEN_SLOTS, QUERY_HEAD_COUNT), minval=0.5, maxval=1.5)
    first_position = jax.random.randint(random_subkeys[5], (QUERY_HEAD_COUNT,), 0, TOKEN_SLOTS)
    position_gap = jax.random.randint(random_subkeys[7], (QUERY_HEAD_COUNT,), 1, TOKEN_SLOTS)
    second_position = (first_position + position_gap) % TOKEN_SLOTS
    group_length = jax.random.uniform(random_subkeys[6], (2, QUERY_HEAD_COUNT), minval=math.log(0.5), maxval=math.log(0.8))
    token_slot_index = jnp.arange(TOKEN_SLOTS)[:, None]
    token_groups = jnp.where(token_slot_index == first_position[None, :], group_length[0][None, :], 0.0)
    token_groups = token_groups + jnp.where(token_slot_index == second_position[None, :], group_length[1][None, :], 0.0)
    return (-head_decay_rate[None, :] * block_multiplier * slot_multiplier + token_groups).astype(jnp.float32)


def soft_pair(key):
    first_key, second_key = jax.random.split(jax.random.fold_in(key, 17))
    queries = jnp.clip(jax.random.normal(first_key, (TOKEN_SLOTS, QUERY_HEAD_COUNT * HEAD_DIM), jnp.float32), -6.0, 6.0)
    keys_drawn = jnp.clip(jax.random.normal(second_key, (TOKEN_SLOTS, KV_HEADS * HEAD_DIM), jnp.float32), -6.0, 6.0)
    return (queries, keys_drawn)


def draw_soft_queries(key, part):
    return soft_pair(key)[0].astype(jnp.bfloat16)


def draw_soft_keys(key, part):
    return soft_pair(key)[1].astype(jnp.bfloat16)


def block_levels(own_key, extent, cuts, least, largest):
    level, own = 1.0, jax.random.fold_in(own_key, 6)
    for dim, blocks in cuts:
        heights = jnp.exp(jax.random.uniform(jax.random.fold_in(own, dim), (blocks,), jnp.float32, least / len(cuts), largest / len(cuts)))
        level = level * jnp.repeat(heights, extent[dim] // blocks).reshape([-1 if axis == dim else 1 for axis in range(len(extent))])
    return level


def profile(amount, total, reach, lean):
    loads = [(1 << 20) // math.isqrt(rank ** lean) + 1 for rank in range(2, amount + 1)]
    rest, given = total - reach - (amount - 1), [1] * (amount - 1)
    while rest > 0:
        movable = [i for i in range(amount - 1) if given[i] < reach]
        mass, remaining = sum([loads[i] for i in movable]), rest
        for i in movable:
            more = min(reach - given[i], max(1, remaining * loads[i] // mass), rest)
            given[i] = given[i] + more
            rest = rest - more
    return np.array([reach] + given)


def uneven(own_key, amount, total, bound, slope):
    if amount == 2:
        one = jax.random.randint(own_key, (), max(1, total - bound), min(bound, total - 1) + 1)
        return jnp.stack([one, total - one])
    tallies = jnp.asarray(profile(amount, total, bound, slope), jnp.int32)
    couples = (amount - 1) // 2
    source_of, receiver = tallies[1:1 + 2 * couples:2], tallies[2:2 + 2 * couples:2]
    slack = jnp.minimum(source_of - 1, bound - receiver)
    passed = jax.random.randint(jax.random.fold_in(own_key, 1), (couples,), 0, 1 << 20) % (slack + 1)
    tallies = tallies.at[1:1 + 2 * couples:2].set(source_of - passed).at[2:2 + 2 * couples:2].set(receiver + passed)
    return tallies[jax.random.permutation(jax.random.fold_in(own_key, 2), amount)]


def centred(key, shape, spread, limit, pieces=(), held_as=jnp.bfloat16):
    array = jax.random.normal(key, shape, jnp.float32) * spread
    if len(pieces) > 0:
        array = block_levels(key, shape, pieces, -0.22, 0.18) * array
    return jnp.clip(array, min=-limit, max=limit).astype(held_as)


def setup_inputs(seed: int = 0, part: int = 0) -> dict:
    streams_of = jax.random.split(jax.random.key(seed), 10)
    own_keys = jax.random.split(jax.random.fold_in(streams_of[9], part), 10)
    return {
        "light_queries": centred(own_keys[0], (TOKEN_SLOTS, QUERY_HEAD_COUNT * HEAD_DIM), 1.0, 6.0, ((0, 16), (1, 8))),
        "light_keys": centred(own_keys[1], (TOKEN_SLOTS, QUERY_HEAD_COUNT * HEAD_DIM), 1.0, 6.0, ((0, 16), (1, 8))),
        "light_values": centred(own_keys[2], (TOKEN_SLOTS, QUERY_HEAD_COUNT * HEAD_DIM), 1.0, 6.0, ((0, 16), (1, 8))),
        "decay_log": draw_decay_log(jax.random.fold_in(jax.random.fold_in(streams_of[9], part), 71), part),
        "norm_gain": jnp.clip(1.0 + 0.15 * jax.random.normal(streams_of[4], (QUERY_HEAD_COUNT * HEAD_DIM,), jnp.float32), 0.25, 1.75),
        "soft_queries": draw_soft_queries(jax.random.fold_in(jax.random.fold_in(streams_of[9], part), 71), part),
        "soft_keys": draw_soft_keys(jax.random.fold_in(jax.random.fold_in(streams_of[9], part), 71), part),
        "soft_values": centred(own_keys[7], (TOKEN_SLOTS, KV_HEADS * HEAD_DIM), 1.0, 6.0, ((0, 16), (1, 8))),
        "lengths": uneven(own_keys[8], N_SEQ, TOKEN_SLOTS * 3 // 4, TOK_DEV, 2).astype(jnp.int32),
    }


EPSILON = 1e-06

def rounded(values):
    return lax.optimization_barrier(values.astype(jnp.bfloat16)).astype(jnp.float32)

def light_reference(light_queries, light_keys, light_values, decay_log, norm_gain, lengths):
    block_shape = (N_SEQ, TOK_DEV, QUERY_HEAD_COUNT, HEAD_DIM)
    queries = light_queries.reshape(block_shape).astype(jnp.float32)
    keys_all = light_keys.reshape(block_shape).astype(jnp.float32)
    values_all = light_values.reshape(block_shape).astype(jnp.float32)
    decays = decay_log.reshape(N_SEQ, TOK_DEV, QUERY_HEAD_COUNT)
    score_scale = HEAD_DIM ** (-0.5)
    token_slot_index = jnp.arange(TOK_DEV, dtype=jnp.int32)
    causal = token_slot_index[:, None] >= token_slot_index[None, :]
    gain_heads = norm_gain.reshape(QUERY_HEAD_COUNT, HEAD_DIM)

    def advance(entering, inputs):
        query_block, key_block, value_block, decay_block, length = inputs
        live_rows = token_slot_index < length
        masked = jnp.where(live_rows[:, None], decay_block, 0.0)
        running = jnp.cumsum(masked, axis=0)
        ending = running[-1]
        scores = jnp.einsum('thd,shd->hts', query_block, key_block)
        log_gaps = running.T[:, :, None] - running.T[:, None, :]
        allowed = causal[None] & live_rows[None, None, :]
        weights = jnp.where(allowed, jnp.exp(jnp.where(causal[None], log_gaps, 0.0)), 0.0)
        intra_weight = rounded(scores * score_scale * weights)
        inside = jnp.einsum('hts,shd->thd', intra_weight, value_block)
        across = jnp.einsum('thd,hde->the', query_block * score_scale, entering, precision=lax.Precision.HIGHEST) * jnp.exp(running)[:, :, None]
        combined = inside + across
        normed = combined * lax.rsqrt(lax.optimization_barrier(jnp.mean(combined * combined, axis=-1, keepdims=True)) + EPSILON) * gain_heads
        output = jnp.where(live_rows[:, None, None], normed, 0.0)
        fading = jnp.exp(ending[None, :] - running) * live_rows[:, None]
        block_keys = rounded(key_block * fading[:, :, None])
        block_state = jnp.einsum('thd,the->hde', block_keys, value_block)
        leaving = jnp.exp(ending)[:, None, None] * entering + block_state
        return (leaving, output)
    initial = jnp.zeros((QUERY_HEAD_COUNT, HEAD_DIM, HEAD_DIM), jnp.float32)
    final_state, outputs = lax.scan(advance, initial, (queries, keys_all, values_all, decays, lengths))
    return outputs.astype(jnp.bfloat16).reshape(TOKEN_SLOTS, QUERY_HEAD_COUNT * HEAD_DIM)

def soft_reference(soft_queries, soft_keys, soft_values, live_all):
    group_size = QUERY_HEAD_COUNT // KV_HEADS
    score_scale = HEAD_DIM ** (-0.5)
    queries = soft_queries.reshape(N_SEQ, TOK_DEV, KV_HEADS, group_size, HEAD_DIM)
    keys_all = soft_keys.reshape(TOKEN_SLOTS, KV_HEADS, HEAD_DIM).transpose(1, 0, 2)
    values_all = soft_values.reshape(TOKEN_SLOTS, KV_HEADS, HEAD_DIM).transpose(1, 0, 2)
    positions = jnp.arange(TOKEN_SLOTS, dtype=jnp.int32)

    def per_block(block_index):
        query_block = lax.dynamic_index_in_dim(queries, block_index, 0, keepdims=False)
        query_pos = block_index * TOK_DEV + jnp.arange(TOK_DEV, dtype=jnp.int32)
        allowed = (positions[None, :] <= query_pos[:, None]) & live_all[None, :]

        def per_head(inputs):
            query_head, key_head, value_head = inputs
            scores = jnp.einsum('tgd,sd->gts', query_head.astype(jnp.float32), key_head.astype(jnp.float32)) * score_scale
            scores = jnp.where(allowed[None], scores, -jnp.inf)
            row_peak = lax.optimization_barrier(jnp.max(scores, axis=-1, keepdims=True))
            probs_full = jnp.exp(scores - row_peak)
            row_total = lax.optimization_barrier(jnp.sum(probs_full, axis=-1))
            summed = jnp.einsum('gts,sd->tgd', rounded(probs_full), value_head.astype(jnp.float32))
            return summed / row_total.T[:, :, None]
        heads_out = lax.map(per_head, (query_block.transpose(1, 0, 2, 3), keys_all, values_all))
        return heads_out.transpose(1, 0, 2, 3).reshape(TOK_DEV, QUERY_HEAD_COUNT * HEAD_DIM)
    outputs = lax.map(per_block, jnp.arange(N_SEQ, dtype=jnp.int32))
    outputs = outputs.reshape(TOKEN_SLOTS, QUERY_HEAD_COUNT * HEAD_DIM)
    return jnp.where(live_all[:, None], outputs, 0.0).astype(jnp.bfloat16)

def reference(light_queries, light_keys, light_values, decay_log, norm_gain, soft_queries, soft_keys, soft_values, lengths):
    positions = jnp.arange(TOKEN_SLOTS, dtype=jnp.int32)
    live_all = positions % TOK_DEV < lengths[positions // TOK_DEV]
    light_out = light_reference(light_queries, light_keys, light_values, decay_log, norm_gain, lengths)
    soft_out = soft_reference(soft_queries, soft_keys, soft_values, live_all)
    return (light_out, soft_out)
```

```python
from functools import partial

import jax
import jax.numpy as jnp
from jax import lax
from jax.experimental import pallas as pl
from jax.experimental.pallas import tpu as pltpu
from jax.sharding import PartitionSpec as P


F32 = jnp.float32
BF16 = jnp.bfloat16
NEG = -1e30
LOG2E = 1.4426950408889634
E_ROWS = 32
VMEM = pl.BlockSpec(memory_space=pltpu.VMEM)
SMEM = pl.BlockSpec(memory_space=pltpu.SMEM)


def call(kernel, out_shape, name, ins, aliases=None, flops=2_000_000, scratch=()):
    specs = [SMEM if s else VMEM for s, unused in ins]
    arrays = [a for unused, a in ins]
    outs = [jax.ShapeDtypeStruct(s, d) for s, d in out_shape]
    return pl.pallas_call(
        kernel,
        out_shape=outs,
        in_specs=specs,
        out_specs=[VMEM] * len(outs),
        scratch_shapes=list(scratch),
        input_output_aliases=aliases or {},
        compiler_params=pltpu.CompilerParams(vmem_limit_bytes=48 * 1024 * 1024),
        cost_estimate=pl.CostEstimate(flops=flops, bytes_accessed=1 << 20, transcendentals=0),
        name=name,
    )(*arrays)


def seq_bits():
    i = lax.axis_index("seq")
    return i, lax.shift_right_logical(i, 3) & 1


def bit(i, level):
    return lax.shift_right_logical(i, level) & 1


def keep_bit(i, level):
    return bit(i, level) ^ bit(i, 3)


def first_head(i, level):
    start = keep_bit(i, 0) * 4
    if level >= 1:
        start += keep_bit(i, 1) * 2
    if level >= 2:
        start += keep_bit(i, 2)
    return start


def put_logs(msg_ref, at, logs):
    hi = logs.astype(BF16)
    rest = logs - hi.astype(F32)
    mid = rest.astype(BF16)
    low = (rest - mid.astype(F32)).astype(BF16)
    both = jnp.concatenate([hi.astype(F32), mid.astype(F32), low.astype(F32), jnp.zeros_like(logs)], axis=0)
    msg_ref[pl.ds(at, E_ROWS), :] = both.astype(BF16)


def get_logs(msg_ref, at):
    rows = msg_ref[pl.ds(at, E_ROWS), :].astype(F32)
    return rows[0:8] + rows[8:16] + rows[16:24]


def prep_kernel(len_ref, k_ref, v_ref, dec_ref, msg_ref, kept_ref, logs_ref, c_ref, ct_ref, states):
    i = lax.axis_index("seq")
    rows = k_ref.shape[0]
    heads = dec_ref.shape[0]
    width = k_ref.shape[1] // heads
    half = heads // 2
    length = len_ref[i]
    lane = lax.broadcasted_iota(jnp.int32, (heads, rows), 1)
    live = lane < length
    masked = jnp.where(live, dec_ref[...], 0.0)
    tri = (
        lax.broadcasted_iota(jnp.int32, (rows, rows), 0)
        <= lax.broadcasted_iota(jnp.int32, (rows, rows), 1)
    ).astype(F32)
    running = jnp.dot(masked, tri, preferred_element_type=F32, precision=lax.Precision.HIGHEST)
    ending = running[:, rows - 1 : rows]
    c_ref[...] = running
    ct_ref[...] = running.T
    logs = jnp.broadcast_to(ending, (heads, 128))
    logs_ref[...] = logs
    fading = jnp.where(live, jnp.exp(ending - running), 0.0)
    for h in range(heads):
        kt = k_ref[:, h * width : (h + 1) * width].T.astype(F32)
        scaled = (kt * fading[h : h + 1, :]).astype(BF16)
        states[h] = jnp.dot(scaled, v_ref[:, h * width : (h + 1) * width], preferred_element_type=F32)
    keep = keep_bit(i, 0) * half
    send = half - keep
    for h in range(half):
        kept_ref[h] = states[keep + h]
        msg_ref[h * width : (h + 1) * width, :] = states[send + h].astype(BF16)
    put_logs(msg_ref, half * width, logs)


def up_kernel(level, recv_ref, kept_ref, logs_ref, msg_ref, next_ref, low_ref, lowlog_ref, sum_ref):
    i = lax.axis_index("seq")
    count, width = kept_ref.shape[0], kept_ref.shape[1]
    upper = bit(i, level) == 1
    own = logs_ref[...]
    other = get_logs(recv_ref, count * width)
    low_logs = jnp.where(upper, other, own)
    lowlog_ref[...] = low_logs
    sum_ref[...] = own + other
    grown = jnp.exp(jnp.where(upper, own, other))
    start = first_head(i, level)
    which = lax.broadcasted_iota(jnp.int32, grown.shape, 0)
    half = count // 2
    keep = keep_bit(i, level + 1) * half
    totals = []
    for h in range(count):
        factor = jnp.sum(jnp.where(which == start + h, grown, 0.0), axis=0, keepdims=True)
        mine = kept_ref[h]
        got = recv_ref[h * width : (h + 1) * width, :].astype(F32)
        low = jnp.where(upper, got, mine)
        high = jnp.where(upper, mine, got)
        low_ref[h] = low
        totals.append(factor * low + high)
    if count == 1:
        msg_ref[...] = totals[0].astype(BF16)
        next_ref[...] = jnp.zeros_like(next_ref)
        return
    first = keep == 0
    for h in range(half):
        next_ref[h] = jnp.where(first, totals[h], totals[half + h])
        msg_ref[h * width : (h + 1) * width, :] = jnp.where(first, totals[half + h], totals[h]).astype(BF16)
    put_logs(msg_ref, half * width, own + other)


def down_kernel(level, top, *refs):
    if top:
        recv_ref, low_ref, lowlog_ref, mine_ref, msg_ref = refs
    else:
        held_ref, recv_ref, low_ref, lowlog_ref, mine_ref, msg_ref = refs
    i = lax.axis_index("seq")
    count, width = low_ref.shape[0], low_ref.shape[1]
    half = count // 2
    upper = bit(i, level) == 1
    grown = jnp.exp(lowlog_ref[...])
    start = first_head(i, level)
    which = lax.broadcasted_iota(jnp.int32, grown.shape, 0)
    if top:
        entering = [recv_ref[...].astype(F32)]
    else:
        first = keep_bit(i, level + 1) == 0
        held = [held_ref[h] for h in range(half)]
        got = [recv_ref[h * width : (h + 1) * width, :].astype(F32) for h in range(half)]
        entering = [jnp.where(first, a, b) for a, b in zip(held, got)]
        entering += [jnp.where(first, b, a) for a, b in zip(held, got)]
    for h in range(count):
        factor = jnp.sum(jnp.where(which == start + h, grown, 0.0), axis=0, keepdims=True)
        low = entering[h]
        high = factor * low + low_ref[h]
        mine_ref[h] = jnp.where(upper, high, low)
        msg_ref[h * width : (h + 1) * width, :] = jnp.where(upper, low, high).astype(BF16)


def inside_kernel(len_ref, q_ref, k_ref, v_ref, c_ref, ct_ref, out_ref):
    i = lax.axis_index("seq")
    rows = q_ref.shape[0]
    heads = c_ref.shape[0]
    width = q_ref.shape[1] // heads
    scale = width ** (-0.5)
    length = len_ref[i]
    row = lax.broadcasted_iota(jnp.int32, (rows, rows), 0)
    col = lax.broadcasted_iota(jnp.int32, (rows, rows), 1)
    allowed = (col <= row) & (col < length)
    running = c_ref[...]
    running_t = ct_ref[...]
    for h in range(heads):
        at = slice(h * width, (h + 1) * width)
        scores = lax.dot_general(
            q_ref[:, at], k_ref[:, at], (((1,), (1,)), ((), ())), preferred_element_type=F32
        )
        gaps = running_t[:, h : h + 1] - running[h : h + 1, :]
        weights = jnp.exp(jnp.where(allowed, gaps, NEG))
        intra = (scores * scale * weights).astype(BF16)
        out_ref[:, at] = jnp.dot(intra, v_ref[:, at], preferred_element_type=F32)


def light_kernel(len_ref, q_ref, inside_ref, held_ref, recv_ref, ct_ref, gain_ref, out_ref):
    i = lax.axis_index("seq")
    rows = q_ref.shape[0]
    half, width = held_ref.shape[0], held_ref.shape[1]
    scale = width ** (-0.5)
    first = keep_bit(i, 0) == 0
    live = lax.broadcasted_iota(jnp.int32, (rows, 1), 0) < len_ref[i]
    grown = jnp.exp(ct_ref[...])
    for h in range(2 * half):
        at = slice(h * width, (h + 1) * width)
        mod = h % half
        held = held_ref[mod].astype(BF16)
        got = recv_ref[mod * width : (mod + 1) * width, :]
        pick_held = first if h < half else jnp.logical_not(first)
        entering = jnp.where(pick_held, held.astype(F32), got.astype(F32)).astype(BF16)
        across = jnp.dot(q_ref[:, at], entering, preferred_element_type=F32) * scale
        combined = inside_ref[:, at] + across * grown[:, h : h + 1]
        mean = jnp.mean(combined * combined, axis=-1, keepdims=True)
        normed = combined * lax.rsqrt(mean + 1e-06) * gain_ref[:, at]
        out_ref[:, at] = jnp.where(live, normed, 0.0).astype(BF16)


def fold(q_ref, keys, values, bias, m_ref, l_ref, acc_ref, fresh):
    heads, rows, width = acc_ref.shape
    factor = width ** (-0.5) * LOG2E

    def one_head(h, carry):
        scores = lax.dot_general(
            q_ref[:, pl.ds(pl.multiple_of(h * width, width), width)],
            keys,
            (((1,), (1,)), ((), ())),
            preferred_element_type=F32,
        )
        scores = scores + bias
        tiles = scores.shape[1] // 128
        peak = jnp.max(scores, axis=-1, keepdims=True)
        if fresh:
            new = jnp.broadcast_to(peak, (rows, 128))
        else:
            old = m_ref[h]
            new = jnp.maximum(old, peak)
        probs = [jnp.exp2((scores[:, t * 128 : (t + 1) * 128] - new) * factor) for t in range(tiles)]
        total = sum(probs[1:], probs[0])
        summed = jnp.dot(
            jnp.concatenate([p.astype(BF16) for p in probs], axis=1), values, preferred_element_type=F32
        )
        if not fresh:
            shrink = jnp.exp2((old - new) * factor)
            total = total + shrink * l_ref[h]
            summed = summed + shrink * acc_ref[h]
        m_ref[h] = new
        l_ref[h] = total
        acc_ref[h] = summed
        return carry

    lax.fori_loop(0, heads, one_head, 0, unroll=2)


def own_kernel(len_ref, q_ref, kv_ref, m_ref, l_ref, acc_ref):
    i = lax.axis_index("seq")
    rows = q_ref.shape[0]
    length = len_ref[i]
    row = lax.broadcasted_iota(jnp.int32, (rows, rows), 0)
    col = lax.broadcasted_iota(jnp.int32, (rows, rows), 1)
    bias = jnp.where((col <= row) & (col < length), 0.0, NEG)
    fold(q_ref, kv_ref[0:rows, :], kv_ref[rows : 2 * rows, :], bias, m_ref, l_ref, acc_ref, True)


def step_kernel(step, count, len_ref, q_ref, *refs):
    last = step == count // 2
    if last:
        f_ref, m_ref, l_ref, acc_ref, out_ref = refs
        blocks = [(f_ref, 0)]
    else:
        f_ref, b_ref, unused_m, unused_l, unused_acc, m_ref, l_ref, acc_ref = refs
        blocks = [(f_ref, 0), (b_ref, count)]
    i = lax.axis_index("seq")
    rows = q_ref.shape[0]
    lane = lax.broadcasted_iota(jnp.int32, (1, rows), 1)

    @pl.when(i >= step)
    def attend():
        biases = []
        for unused, wrap in blocks:
            block = i - step if wrap == 0 else i + step - wrap
            length = jnp.where(block >= 0, len_ref[jnp.maximum(block, 0)], 0)
            biases.append(jnp.where(lane < length, 0.0, NEG))
        keys = [ref[0:rows, :] for ref, unused in blocks]
        values = [ref[rows : 2 * rows, :] for ref, unused in blocks]
        fold(
            q_ref,
            jnp.concatenate(keys, axis=0),
            jnp.concatenate(values, axis=0),
            jnp.concatenate(biases, axis=1),
            m_ref,
            l_ref,
            acc_ref,
            False,
        )

    if last:
        live = lax.broadcasted_iota(jnp.int32, (rows, 1), 0) < len_ref[i]
        width = acc_ref.shape[2]
        for h in range(acc_ref.shape[0]):
            total = jnp.sum(l_ref[h], axis=-1, keepdims=True)
            result = acc_ref[h] / total
            out_ref[:, h * width : (h + 1) * width] = jnp.where(live, result, 0.0).astype(BF16)


def body(
    light_queries,
    light_keys,
    light_values,
    decay_log,
    norm_gain,
    soft_queries,
    soft_keys,
    soft_values,
    lengths,
):
    rows = light_queries.shape[0]
    heads = decay_log.shape[1]
    width = light_queries.shape[1] // heads
    count = lax.axis_size("seq")
    half = heads // 2
    forward = [(i, (i + 1) % count) for i in range(count)]
    backward = [(i, (i - 1) % count) for i in range(count)]

    def exchange(x, distance):
        return lax.ppermute(x, "seq", [(i, i ^ distance) for i in range(count)])

    lens = (True, lengths)
    own_kv = jnp.concatenate([soft_keys, soft_values], axis=0)
    f = lax.ppermute(own_kv, "seq", forward)
    b = lax.ppermute(own_kv, "seq", backward)

    msg, kept, logs, running, running_t = call(
        prep_kernel,
        [
            ((half * width + E_ROWS, width), BF16),
            ((half, width, width), F32),
            ((heads, 128), F32),
            ((heads, rows), F32),
            ((rows, heads), F32),
        ],
        "prep",
        [lens, (False, light_keys), (False, light_values), (False, decay_log.T)],
        scratch=[pltpu.VMEM((heads, width, width), F32)],
    )
    saved = []
    n = half
    for level in range(3):
        recv = exchange(msg, 1 << level)
        m = max(n // 2, 1)
        tail = E_ROWS if n > 1 else 0
        msg, nxt, low, low_logs, new_logs = call(
            partial(up_kernel, level),
            [
                ((m * width + tail, width), BF16),
                ((m, width, width), F32),
                ((n, width, width), F32),
                ((heads, 128), F32),
                ((heads, 128), F32),
            ],
            "up",
            [(False, recv), (False, kept), (False, logs)],
        )
        saved.append((low, low_logs))
        kept, logs, n = (nxt, new_logs, n // 2)
    recv = lax.ppermute(msg, "seq", [(i, count - 1 - i) for i in range(count // 2)])
    held = None
    for level in (2, 1, 0):
        low, low_logs = saved[level]
        n = low.shape[0]
        ins = [(False, recv), (False, low), (False, low_logs)]
        if held is not None:
            ins = [(False, held)] + ins
        held, msg = call(
            partial(down_kernel, level, held is None),
            [((n, width, width), F32), ((n * width, width), BF16)],
            "down",
            ins,
        )
        recv = exchange(msg, 1 << level)
    (inside,) = call(
        inside_kernel,
        [((rows, heads * width), F32)],
        "inside",
        [
            lens,
            (False, light_queries),
            (False, light_keys),
            (False, light_values),
            (False, running),
            (False, running_t),
        ],
    )
    (light_out,) = call(
        light_kernel,
        [((rows, heads * width), BF16)],
        "light",
        [
            lens,
            (False, light_queries),
            (False, inside),
            (False, held),
            (False, recv),
            (False, running_t),
            (False, norm_gain.reshape(1, heads * width)),
        ],
    )

    soft_heads = soft_queries.shape[1] // width
    stat = ((soft_heads, rows, 128), F32)
    state = call(
        own_kernel,
        [stat, stat, stat],
        "own",
        [lens, (False, soft_queries), (False, own_kv)],
    )
    for step in range(1, count // 2):
        nf = lax.ppermute(f, "seq", forward)
        nb = lax.ppermute(b, "seq", backward) if step + 1 < count // 2 else None
        state = call(
            partial(step_kernel, step, count),
            [stat, stat, stat],
            "step",
            [lens, (False, soft_queries), (False, f), (False, b)] + [(False, s) for s in state],
            aliases={4: 0, 5: 1, 6: 2},
        )
        f, b = nf, nb
    (soft_out,) = call(
        partial(step_kernel, count // 2, count),
        [((rows, soft_heads * width), BF16)],
        "last",
        [lens, (False, soft_queries), (False, f)] + [(False, s) for s in state],
    )
    return (light_out, soft_out)


def solution(mesh):
    return jax.shard_map(
        body,
        mesh=mesh,
        in_specs=(
            P(("groups", "seq"), ("section", "mp")),
            P(("groups", "seq"), ("section", "mp")),
            P(("groups", "seq"), ("section", "mp")),
            P(("groups", "seq"), ("section", "mp")),
            P(("section", "mp")),
            P(("groups", "seq"), ("section", "mp")),
            P(("groups", "seq"), ("section", "mp")),
            P(("groups", "seq"), ("section", "mp")),
            P("groups"),
        ),
        out_specs=(
            P(("groups", "seq"), ("section", "mp")),
            P(("groups", "seq"), ("section", "mp")),
        ),
        check_vma=False,
    )
```

```python
from functools import partial

import jax
import jax.numpy as jnp
from jax import lax
from jax.experimental import pallas as pl
from jax.experimental.pallas import tpu as pltpu
from jax.sharding import PartitionSpec as P


F32 = jnp.float32
BF16 = jnp.bfloat16
NEG = -1e30
LOG2E = 1.4426950408889634
E_ROWS = 32
VMEM = pl.BlockSpec(memory_space=pltpu.VMEM)
SMEM = pl.BlockSpec(memory_space=pltpu.SMEM)


def call(kernel, out_shape, ins, aliases=None, flops=2_000_000, scratch=()):
    specs = [SMEM if s else VMEM for s, unused in ins]
    arrays = [a for unused, a in ins]
    outs = [jax.ShapeDtypeStruct(s, d) for s, d in out_shape]
    return pl.pallas_call(
        kernel,
        out_shape=outs,
        in_specs=specs,
        out_specs=[VMEM] * len(outs),
        scratch_shapes=list(scratch),
        input_output_aliases=aliases or {},
        compiler_params=pltpu.CompilerParams(vmem_limit_bytes=48 * 1024 * 1024),
        cost_estimate=pl.CostEstimate(flops=flops, bytes_accessed=1 << 20, transcendentals=0),
    )(*arrays)


def bit(i, level):
    return lax.shift_right_logical(i, level) & 1


def keep_bit(i, level):
    return bit(i, level) ^ (bit(i, 3) if level == 2 else 0)


def first_head(i, level):
    start = keep_bit(i, 0) * 4
    if level >= 1:
        start += keep_bit(i, 1) * 2
    if level >= 2:
        start += keep_bit(i, 2)
    return start


def put_logs(msg_ref, at, logs):
    hi = logs.astype(BF16)
    rest = logs - hi.astype(F32)
    mid = rest.astype(BF16)
    low = (rest - mid.astype(F32)).astype(BF16)
    both = jnp.concatenate([hi.astype(F32), mid.astype(F32), low.astype(F32), jnp.zeros_like(logs)], axis=0)
    msg_ref[pl.ds(at, E_ROWS), :] = both.astype(BF16)


def get_logs(msg_ref, at):
    rows = msg_ref[pl.ds(at, E_ROWS), :].astype(F32)
    return rows[0:8] + rows[8:16] + rows[16:24]


def prep_kernel(len_ref, k_ref, v_ref, dec_ref, msg_ref, kept_ref, logs_ref, c_ref, ct_ref, states):
    i = lax.axis_index("seq")
    rows = k_ref.shape[0]
    heads = dec_ref.shape[0]
    width = k_ref.shape[1] // heads
    half = heads // 2
    length = len_ref[i]
    lane = lax.broadcasted_iota(jnp.int32, (heads, rows), 1)
    live = lane < length
    masked = jnp.where(live, dec_ref[...], 0.0)
    tri = (
        lax.broadcasted_iota(jnp.int32, (rows, rows), 0)
        <= lax.broadcasted_iota(jnp.int32, (rows, rows), 1)
    ).astype(F32)
    running = jnp.dot(masked, tri, preferred_element_type=F32, precision=lax.Precision.HIGHEST)
    ending = running[:, rows - 1 : rows]
    c_ref[...] = running
    ct_ref[...] = running.T
    logs = jnp.broadcast_to(ending, (heads, 128))
    logs_ref[...] = logs
    fading = jnp.where(live, jnp.exp(ending - running), 0.0)
    for h in range(heads):
        kt = k_ref[:, h * width : (h + 1) * width].T.astype(F32)
        scaled = (kt * fading[h : h + 1, :]).astype(BF16)
        states[h] = jnp.dot(scaled, v_ref[:, h * width : (h + 1) * width], preferred_element_type=F32)
    keep = keep_bit(i, 0) * half
    send = half - keep
    for h in range(half):
        kept_ref[h] = states[keep + h]
        msg_ref[h * width : (h + 1) * width, :] = states[send + h].astype(BF16)
    put_logs(msg_ref, half * width, logs)


def up_kernel(level, recv_ref, kept_ref, logs_ref, msg_ref, next_ref, low_ref, lowlog_ref, sum_ref):
    i = lax.axis_index("seq")
    count, width = kept_ref.shape[0], kept_ref.shape[1]
    upper = bit(i, level) == 1
    own = logs_ref[...]
    other = get_logs(recv_ref, count * width)
    low_logs = jnp.where(upper, other, own)
    lowlog_ref[...] = low_logs
    sum_ref[...] = own + other
    grown = jnp.exp(jnp.where(upper, own, other))
    start = first_head(i, level)
    which = lax.broadcasted_iota(jnp.int32, grown.shape, 0)
    half = count // 2
    keep = keep_bit(i, level + 1) * half
    totals = []
    for h in range(count):
        factor = jnp.sum(jnp.where(which == start + h, grown, 0.0), axis=0, keepdims=True)
        mine = kept_ref[h]
        got = recv_ref[h * width : (h + 1) * width, :].astype(F32)
        low = jnp.where(upper, got, mine)
        high = jnp.where(upper, mine, got)
        low_ref[h] = low
        totals.append(factor * low + high)
    if count == 1:
        msg_ref[...] = totals[0].astype(BF16)
        next_ref[...] = jnp.zeros_like(next_ref)
        return
    first = keep == 0
    for h in range(half):
        next_ref[h] = jnp.where(first, totals[h], totals[half + h])
        msg_ref[h * width : (h + 1) * width, :] = jnp.where(first, totals[half + h], totals[h]).astype(BF16)
    put_logs(msg_ref, half * width, own + other)


def down_kernel(level, top, *refs):
    if top:
        recv_ref, low_ref, lowlog_ref, mine_ref, msg_ref = refs
    else:
        held_ref, recv_ref, low_ref, lowlog_ref, mine_ref, msg_ref = refs
    i = lax.axis_index("seq")
    count, width = low_ref.shape[0], low_ref.shape[1]
    half = count // 2
    upper = bit(i, level) == 1
    grown = jnp.exp(lowlog_ref[...])
    start = first_head(i, level)
    which = lax.broadcasted_iota(jnp.int32, grown.shape, 0)
    if top:
        entering = [recv_ref[...].astype(F32)]
    else:
        first = keep_bit(i, level + 1) == 0
        held = [held_ref[h] for h in range(half)]
        got = [recv_ref[h * width : (h + 1) * width, :].astype(F32) for h in range(half)]
        entering = [jnp.where(first, a, b) for a, b in zip(held, got)]
        entering += [jnp.where(first, b, a) for a, b in zip(held, got)]
    for h in range(count):
        factor = jnp.sum(jnp.where(which == start + h, grown, 0.0), axis=0, keepdims=True)
        low = entering[h]
        high = factor * low + low_ref[h]
        mine_ref[h] = jnp.where(upper, high, low)
        msg_ref[h * width : (h + 1) * width, :] = jnp.where(upper, low, high).astype(BF16)


def inside_kernel(len_ref, q_ref, k_ref, v_ref, c_ref, ct_ref, out_ref):
    i = lax.axis_index("seq")
    rows = q_ref.shape[0]
    heads = c_ref.shape[0]
    width = q_ref.shape[1] // heads
    scale = width ** (-0.5)
    length = len_ref[i]
    row = lax.broadcasted_iota(jnp.int32, (rows, rows), 0)
    col = lax.broadcasted_iota(jnp.int32, (rows, rows), 1)
    allowed = (col <= row) & (col < length)
    running = c_ref[...]
    running_t = ct_ref[...]
    for h in range(heads):
        at = slice(h * width, (h + 1) * width)
        scores = lax.dot_general(
            q_ref[:, at], k_ref[:, at], (((1,), (1,)), ((), ())), preferred_element_type=F32
        )
        gaps = running_t[:, h : h + 1] - running[h : h + 1, :]
        weights = jnp.exp(jnp.where(allowed, gaps, NEG))
        intra = (scores * scale * weights).astype(BF16)
        out_ref[:, at] = jnp.dot(intra, v_ref[:, at], preferred_element_type=F32)


def light_kernel(len_ref, q_ref, inside_ref, held_ref, recv_ref, ct_ref, gain_ref, out_ref):
    i = lax.axis_index("seq")
    rows = q_ref.shape[0]
    half, width = held_ref.shape[0], held_ref.shape[1]
    scale = width ** (-0.5)
    first = keep_bit(i, 0) == 0
    live = lax.broadcasted_iota(jnp.int32, (rows, 1), 0) < len_ref[i]
    grown = jnp.exp(ct_ref[...])
    for h in range(2 * half):
        at = slice(h * width, (h + 1) * width)
        mod = h % half
        held = held_ref[mod].astype(BF16)
        got = recv_ref[mod * width : (mod + 1) * width, :]
        pick_held = first if h < half else jnp.logical_not(first)
        entering = jnp.where(pick_held, held.astype(F32), got.astype(F32)).astype(BF16)
        across = jnp.dot(q_ref[:, at], entering, preferred_element_type=F32) * scale
        combined = inside_ref[:, at] + across * grown[:, h : h + 1]
        mean = jnp.mean(combined * combined, axis=-1, keepdims=True)
        normed = combined * lax.rsqrt(mean + 1e-06) * gain_ref[:, at]
        out_ref[:, at] = jnp.where(live, normed, 0.0).astype(BF16)


def unit_columns(rows):
    return jnp.where(lax.broadcasted_iota(jnp.int32, (rows, 128), 1) == 0, 1.0, 0.0).astype(BF16)


def own_kernel(len_ref, q_ref, k_ref, v_ref, q2_ref, m_ref, l_ref, acc_ref):
    i = lax.axis_index("seq")
    rows, width = k_ref.shape
    heads = q_ref.shape[1] // width
    factor = width ** (-0.5) * LOG2E
    q2_ref[:, width:] = unit_columns(heads * rows)
    for h in range(heads):
        q2_ref[h * rows : (h + 1) * rows, :width] = q_ref[:, h * width : (h + 1) * width]
    row = lax.broadcasted_iota(jnp.int32, (rows, rows), 0)
    col = lax.broadcasted_iota(jnp.int32, (rows, rows), 1)
    allowed = (col <= row) & (col < len_ref[i])
    scores = jnp.dot(q2_ref[:, :width], k_ref[...].T, preferred_element_type=F32)
    scores = jnp.where(allowed[None], scores.reshape(heads, rows, rows), NEG).reshape(heads * rows, rows)
    peak = jnp.broadcast_to(jnp.max(scores, axis=-1, keepdims=True), (heads * rows, 128))
    probs = [jnp.exp2((scores[:, t : t + 128] - peak) * factor) for t in range(0, rows, 128)]
    m_ref[...] = peak
    l_ref[...] = sum(probs[1:], probs[0])
    acc_ref[...] = jnp.dot(
        jnp.concatenate([p.astype(BF16) for p in probs], axis=1), v_ref[...], preferred_element_type=F32
    )


def attend(q2_ref, blocks, lengths, old_ref):
    rows, width = blocks[0].shape[0] // 2, blocks[0].shape[1]
    factor = width ** (-0.5) * LOG2E
    row = lax.broadcasted_iota(jnp.int32, (128, rows), 0)
    col = lax.broadcasted_iota(jnp.int32, (128, rows), 1)
    biases = [jnp.where((row == 0) & (col >= n), NEG, 0.0).astype(BF16) for n in lengths]
    keys_t = jnp.concatenate([ref[0:rows, :].T for ref in blocks], axis=1)
    keys_t = jnp.concatenate([keys_t, jnp.concatenate(biases, axis=1)], axis=0)
    values = jnp.concatenate([ref[rows : 2 * rows, :] for ref in blocks], axis=0)
    scores = jnp.dot(q2_ref[...], keys_t, preferred_element_type=F32)
    old = old_ref[...]
    new = jnp.maximum(old, jnp.max(scores, axis=-1, keepdims=True))
    probs = [jnp.exp2((scores[:, t : t + 128] - new) * factor) for t in range(0, scores.shape[1], 128)]
    summed = jnp.dot(
        jnp.concatenate([p.astype(BF16) for p in probs], axis=1), values, preferred_element_type=F32
    )
    return new, jnp.exp2((old - new) * factor), sum(probs[1:], probs[0]), summed


def step_kernel(step, count, len_ref, q2_ref, f_ref, b_ref, unused_m, unused_l, unused_acc, m_ref, l_ref, acc_ref):
    i = lax.axis_index("seq")

    @pl.when(i >= step)
    def run():
        wrapped = i + step - count
        lengths = [
            len_ref[jnp.maximum(i - step, 0)],
            jnp.where(wrapped >= 0, len_ref[jnp.maximum(wrapped, 0)], 0),
        ]
        new, shrink, total, summed = attend(q2_ref, [f_ref, b_ref], lengths, m_ref)
        m_ref[...] = new
        l_ref[...] = shrink * l_ref[...] + total
        acc_ref[...] = shrink * acc_ref[...] + summed


def last_kernel(step, len_ref, q2_ref, f_ref, m_ref, l_ref, acc_ref, out_ref):
    i = lax.axis_index("seq")
    rows, width = f_ref.shape[0] // 2, f_ref.shape[1]
    heads = q2_ref.shape[0] // rows
    live = lax.broadcasted_iota(jnp.int32, (rows, 1), 0) < len_ref[i]

    def finish(total, summed):
        result = summed / jnp.sum(total, axis=-1, keepdims=True)
        for h in range(heads):
            picked = jnp.where(live, result[h * rows : (h + 1) * rows, :], 0.0)
            out_ref[:, h * width : (h + 1) * width] = picked.astype(BF16)

    @pl.when(i >= step)
    def run():
        _, shrink, total, summed = attend(q2_ref, [f_ref], [len_ref[jnp.maximum(i - step, 0)]], m_ref)
        finish(shrink * l_ref[...] + total, shrink * acc_ref[...] + summed)

    @pl.when(i < step)
    def skip():
        finish(l_ref[...], acc_ref[...])


def body(
    light_queries,
    light_keys,
    light_values,
    decay_log,
    norm_gain,
    soft_queries,
    soft_keys,
    soft_values,
    lengths,
):
    rows = light_queries.shape[0]
    heads = decay_log.shape[1]
    width = light_queries.shape[1] // heads
    count = lax.axis_size("seq")
    half = heads // 2
    forward = [(i, (i + 1) % count) for i in range(count)]
    backward = [(i, (i - 1) % count) for i in range(count)]

    def send(x, pairs):
        return lax.ppermute(x, "seq", pairs)

    def exchange(x, distance):
        return send(x, [(i, i ^ distance) for i in range(count)])

    lens = (True, lengths)
    own_kv = jnp.concatenate([soft_keys, soft_values], axis=0)
    f = send(own_kv, forward)
    b = send(own_kv, backward)

    msg, kept, logs, running, running_t = call(
        prep_kernel,
        [
            ((half * width + E_ROWS, width), BF16),
            ((half, width, width), F32),
            ((heads, 128), F32),
            ((heads, rows), F32),
            ((rows, heads), F32),
        ],
        [lens, (False, light_keys), (False, light_values), (False, decay_log.T)],
        scratch=[pltpu.VMEM((heads, width, width), F32)],
    )
    saved = []
    n = half
    for level in range(3):
        recv = exchange(msg, 1 << level)
        m = max(n // 2, 1)
        tail = E_ROWS if n > 1 else 0
        msg, nxt, low, low_logs, new_logs = call(
            partial(up_kernel, level),
            [
                ((m * width + tail, width), BF16),
                ((m, width, width), F32),
                ((n, width, width), F32),
                ((heads, 128), F32),
                ((heads, 128), F32),
            ],
            [(False, recv), (False, kept), (False, logs)],
        )
        saved.append((low, low_logs))
        kept, logs, n = (nxt, new_logs, n // 2)
    recv = send(msg, [(i, (i + 4 if i >= 4 else i - 4) % count) for i in range(count // 2)])
    held = None
    for level in (2, 1, 0):
        low, low_logs = saved[level]
        n = low.shape[0]
        ins = [(False, recv), (False, low), (False, low_logs)]
        if held is not None:
            ins = [(False, held)] + ins
        held, msg = call(
            partial(down_kernel, level, held is None),
            [((n, width, width), F32), ((n * width, width), BF16)],
            ins,
        )
        recv = exchange(msg, 1 << level)
    (inside,) = call(
        inside_kernel,
        [((rows, heads * width), F32)],
        [
            lens,
            (False, light_queries),
            (False, light_keys),
            (False, light_values),
            (False, running),
            (False, running_t),
        ],
    )
    (light_out,) = call(
        light_kernel,
        [((rows, heads * width), BF16)],
        [
            lens,
            (False, light_queries),
            (False, inside),
            (False, held),
            (False, recv),
            (False, running_t),
            (False, norm_gain.reshape(1, heads * width)),
        ],
    )

    soft_rows = soft_queries.shape[1] // width * rows
    stat = ((soft_rows, 128), F32)
    q2, *state = call(
        own_kernel,
        [((soft_rows, width + 128), BF16), stat, stat, stat],
        [lens, (False, soft_queries), (False, soft_keys), (False, soft_values)],
    )
    for step in range(1, count // 2):
        nf = send(f, forward)
        nb = send(b, backward) if step + 1 < count // 2 else None
        state = call(
            partial(step_kernel, step, count),
            [stat, stat, stat],
            [lens, (False, q2), (False, f), (False, b)] + [(False, s) for s in state],
            aliases={4: 0, 5: 1, 6: 2},
        )
        f, b = nf, nb
    (soft_out,) = call(
        partial(last_kernel, count // 2),
        [((rows, soft_queries.shape[1]), BF16)],
        [lens, (False, q2), (False, f)] + [(False, s) for s in state],
    )
    return (light_out, soft_out)


def solution(mesh):
    return jax.shard_map(
        body,
        mesh=mesh,
        in_specs=(
            P(("groups", "seq"), ("section", "mp")),
            P(("groups", "seq"), ("section", "mp")),
            P(("groups", "seq"), ("section", "mp")),
            P(("groups", "seq"), ("section", "mp")),
            P(("section", "mp")),
            P(("groups", "seq"), ("section", "mp")),
            P(("groups", "seq"), ("section", "mp")),
            P(("groups", "seq"), ("section", "mp")),
            P("groups"),
        ),
        out_specs=(
            P(("groups", "seq"), ("section", "mp")),
            P(("groups", "seq"), ("section", "mp")),
        ),
        check_vma=False,
    )
```

```python
from functools import partial

import jax
import jax.numpy as jnp
from jax import lax
from jax.experimental import pallas as pl
from jax.experimental.pallas import tpu as pltpu
from jax.sharding import PartitionSpec as P


F32 = jnp.float32
BF16 = jnp.bfloat16
NEG = -1e30
LOG2E = 1.4426950408889634
E_ROWS = 32
VMEM = pl.BlockSpec(memory_space=pltpu.VMEM)
ANY = pl.BlockSpec(memory_space=pltpu.HBM)
SMEM = pl.BlockSpec(memory_space=pltpu.SMEM)


def call(kernel, out_shape, ins, aliases=None, flops=2_000_000, scratch=()):
    specs = [ANY if s is None else SMEM if s else VMEM for s, unused in ins]
    arrays = [a for unused, a in ins]
    outs = [jax.ShapeDtypeStruct(s, d) for s, d in out_shape]
    return pl.pallas_call(
        kernel,
        out_shape=outs,
        in_specs=specs,
        out_specs=[VMEM] * len(outs),
        scratch_shapes=list(scratch),
        input_output_aliases=aliases or {},
        compiler_params=pltpu.CompilerParams(vmem_limit_bytes=48 * 1024 * 1024),
        cost_estimate=pl.CostEstimate(flops=flops, bytes_accessed=1 << 20, transcendentals=0),
    )(*arrays)


def bit(i, level):
    return lax.shift_right_logical(i, level) & 1


def keep_bit(i, level):
    return bit(i, level) ^ (bit(i, 3) if level == 2 else 0)


def first_head(i, level):
    start = keep_bit(i, 0) * 4
    if level >= 1:
        start += keep_bit(i, 1) * 2
    if level >= 2:
        start += keep_bit(i, 2)
    return start


def put_logs(msg_ref, at, logs):
    hi = logs.astype(BF16)
    rest = logs - hi.astype(F32)
    mid = rest.astype(BF16)
    low = (rest - mid.astype(F32)).astype(BF16)
    both = jnp.concatenate([hi.astype(F32), mid.astype(F32), low.astype(F32), jnp.zeros_like(logs)], axis=0)
    msg_ref[pl.ds(at, E_ROWS), :] = both.astype(BF16)


def get_logs(msg_ref, at):
    rows = msg_ref[pl.ds(at, E_ROWS), :].astype(F32)
    return rows[0:8] + rows[8:16] + rows[16:24]


def prep_kernel(len_ref, k_hbm, v_hbm, dec_ref, msg_ref, kept_ref, logs_ref, c_ref, ct_ref, states, k_ref, v_ref, sems):
    k_copy = pltpu.make_async_copy(k_hbm, k_ref, sems.at[0])
    v_copy = pltpu.make_async_copy(v_hbm, v_ref, sems.at[1])
    k_copy.start()
    v_copy.start()
    i = lax.axis_index("seq")
    rows = k_ref.shape[0]
    heads = dec_ref.shape[0]
    width = k_ref.shape[1] // heads
    half = heads // 2
    length = len_ref[i]
    lane = lax.broadcasted_iota(jnp.int32, (heads, rows), 1)
    live = lane < length
    masked = jnp.where(live, dec_ref[...], 0.0)
    tri = (
        lax.broadcasted_iota(jnp.int32, (rows, rows), 0)
        <= lax.broadcasted_iota(jnp.int32, (rows, rows), 1)
    ).astype(F32)
    running = jnp.dot(masked, tri, preferred_element_type=F32, precision=lax.Precision.HIGHEST)
    ending = running[:, rows - 1 : rows]
    c_ref[...] = running
    ct_ref[...] = running.T
    logs = jnp.broadcast_to(ending, (heads, 128))
    logs_ref[...] = logs
    fading = jnp.where(live, jnp.exp(ending - running), 0.0)
    k_copy.wait()
    v_copy.wait()
    for h in range(heads):
        kt = k_ref[:, h * width : (h + 1) * width].T.astype(F32)
        scaled = (kt * fading[h : h + 1, :]).astype(BF16)
        states[h] = jnp.dot(scaled, v_ref[:, h * width : (h + 1) * width], preferred_element_type=F32)
    keep = keep_bit(i, 0) * half
    send = half - keep
    for h in range(half):
        kept_ref[h] = states[keep + h]
        msg_ref[h * width : (h + 1) * width, :] = states[send + h].astype(BF16)
    put_logs(msg_ref, half * width, logs)


def up_kernel(level, recv_ref, kept_ref, logs_ref, msg_ref, next_ref, low_ref, lowlog_ref, sum_ref):
    i = lax.axis_index("seq")
    count, width = kept_ref.shape[0], kept_ref.shape[1]
    upper = bit(i, level) == 1
    own = logs_ref[...]
    other = get_logs(recv_ref, count * width)
    low_logs = jnp.where(upper, other, own)
    lowlog_ref[...] = low_logs
    sum_ref[...] = own + other
    grown = jnp.exp(jnp.where(upper, own, other))
    start = first_head(i, level)
    which = lax.broadcasted_iota(jnp.int32, grown.shape, 0)
    half = count // 2
    keep = keep_bit(i, level + 1) * half
    totals = []
    for h in range(count):
        factor = jnp.sum(jnp.where(which == start + h, grown, 0.0), axis=0, keepdims=True)
        mine = kept_ref[h]
        got = recv_ref[h * width : (h + 1) * width, :].astype(F32)
        low = jnp.where(upper, got, mine)
        high = jnp.where(upper, mine, got)
        low_ref[h] = low
        totals.append(factor * low + high)
    if count == 1:
        msg_ref[...] = totals[0].astype(BF16)
        next_ref[...] = jnp.zeros_like(next_ref)
        return
    first = keep == 0
    for h in range(half):
        next_ref[h] = jnp.where(first, totals[h], totals[half + h])
        msg_ref[h * width : (h + 1) * width, :] = jnp.where(first, totals[half + h], totals[h]).astype(BF16)
    put_logs(msg_ref, half * width, own + other)


def down_kernel(level, top, *refs):
    if top:
        recv_ref, low_ref, lowlog_ref, mine_ref, msg_ref = refs
    else:
        held_ref, recv_ref, low_ref, lowlog_ref, mine_ref, msg_ref = refs
    i = lax.axis_index("seq")
    count, width = low_ref.shape[0], low_ref.shape[1]
    half = count // 2
    upper = bit(i, level) == 1
    grown = jnp.exp(lowlog_ref[...])
    start = first_head(i, level)
    which = lax.broadcasted_iota(jnp.int32, grown.shape, 0)
    if top:
        entering = [recv_ref[...].astype(F32)]
    else:
        first = keep_bit(i, level + 1) == 0
        held = [held_ref[h] for h in range(half)]
        got = [recv_ref[h * width : (h + 1) * width, :].astype(F32) for h in range(half)]
        entering = [jnp.where(first, a, b) for a, b in zip(held, got)]
        entering += [jnp.where(first, b, a) for a, b in zip(held, got)]
    for h in range(count):
        factor = jnp.sum(jnp.where(which == start + h, grown, 0.0), axis=0, keepdims=True)
        low = entering[h]
        high = factor * low + low_ref[h]
        mine_ref[h] = jnp.where(upper, high, low)
        msg_ref[h * width : (h + 1) * width, :] = jnp.where(upper, low, high).astype(BF16)


def inside_kernel(len_ref, q_ref, k_ref, v_ref, c_ref, ct_ref, out_ref):
    i = lax.axis_index("seq")
    rows = q_ref.shape[0]
    heads = c_ref.shape[0]
    width = q_ref.shape[1] // heads
    scale = width ** (-0.5)
    length = len_ref[i]
    row = lax.broadcasted_iota(jnp.int32, (rows, rows), 0)
    col = lax.broadcasted_iota(jnp.int32, (rows, rows), 1)
    allowed = (col <= row) & (col < length)
    running = c_ref[...]
    running_t = ct_ref[...]
    for h in range(heads):
        at = slice(h * width, (h + 1) * width)
        scores = lax.dot_general(
            q_ref[:, at], k_ref[:, at], (((1,), (1,)), ((), ())), preferred_element_type=F32
        )
        gaps = running_t[:, h : h + 1] - running[h : h + 1, :]
        weights = jnp.exp(jnp.where(allowed, gaps, NEG))
        intra = (scores * scale * weights).astype(BF16)
        out_ref[:, at] = jnp.dot(intra, v_ref[:, at], preferred_element_type=F32)


def light_kernel(len_ref, q_ref, inside_ref, held_ref, recv_ref, ct_ref, gain_ref, out_ref):
    i = lax.axis_index("seq")
    rows = q_ref.shape[0]
    half, width = held_ref.shape[0], held_ref.shape[1]
    scale = width ** (-0.5)
    first = keep_bit(i, 0) == 0
    live = lax.broadcasted_iota(jnp.int32, (rows, 1), 0) < len_ref[i]
    grown = jnp.exp(ct_ref[...])
    for h in range(2 * half):
        at = slice(h * width, (h + 1) * width)
        mod = h % half
        held = held_ref[mod].astype(BF16)
        got = recv_ref[mod * width : (mod + 1) * width, :]
        pick_held = first if h < half else jnp.logical_not(first)
        entering = jnp.where(pick_held, held.astype(F32), got.astype(F32)).astype(BF16)
        across = jnp.dot(q_ref[:, at], entering, preferred_element_type=F32) * scale
        combined = inside_ref[:, at] + across * grown[:, h : h + 1]
        mean = jnp.mean(combined * combined, axis=-1, keepdims=True)
        normed = combined * lax.rsqrt(mean + 1e-06) * gain_ref[:, at]
        out_ref[:, at] = jnp.where(live, normed, 0.0).astype(BF16)


def unit_columns(rows):
    return jnp.where(lax.broadcasted_iota(jnp.int32, (rows, 128), 1) == 0, 1.0, 0.0).astype(BF16)


def own_kernel(len_ref, q_ref, k_ref, v_ref, q2_ref, m_ref, l_ref, acc_ref):
    i = lax.axis_index("seq")
    rows, width = k_ref.shape
    heads = q_ref.shape[1] // width
    factor = width ** (-0.5) * LOG2E
    q2_ref[:, width:] = unit_columns(heads * rows)
    for h in range(heads):
        q2_ref[h * rows : (h + 1) * rows, :width] = q_ref[:, h * width : (h + 1) * width]
    row = lax.broadcasted_iota(jnp.int32, (rows, rows), 0)
    col = lax.broadcasted_iota(jnp.int32, (rows, rows), 1)
    allowed = (col <= row) & (col < len_ref[i])
    scores = jnp.dot(q2_ref[:, :width], k_ref[...].T, preferred_element_type=F32)
    scores = jnp.where(allowed[None], scores.reshape(heads, rows, rows), NEG).reshape(heads * rows, rows)
    peak = jnp.broadcast_to(jnp.max(scores, axis=-1, keepdims=True), (heads * rows, 128))
    probs = [jnp.exp2((scores[:, t : t + 128] - peak) * factor) for t in range(0, rows, 128)]
    m_ref[...] = peak
    l_ref[...] = sum(probs[1:], probs[0])
    acc_ref[...] = jnp.dot(
        jnp.concatenate([p.astype(BF16) for p in probs], axis=1), v_ref[...], preferred_element_type=F32
    )


def attend(q2_ref, blocks, lengths, old_ref):
    rows, width = blocks[0].shape[0] // 2, blocks[0].shape[1]
    factor = width ** (-0.5) * LOG2E
    row = lax.broadcasted_iota(jnp.int32, (128, rows), 0)
    col = lax.broadcasted_iota(jnp.int32, (128, rows), 1)
    biases = [jnp.where((row == 0) & (col >= n), NEG, 0.0).astype(BF16) for n in lengths]
    keys_t = jnp.concatenate([ref[0:rows, :].T for ref in blocks], axis=1)
    keys_t = jnp.concatenate([keys_t, jnp.concatenate(biases, axis=1)], axis=0)
    values = jnp.concatenate([ref[rows : 2 * rows, :] for ref in blocks], axis=0)
    scores = jnp.dot(q2_ref[...], keys_t, preferred_element_type=F32)
    old = old_ref[...]
    new = jnp.maximum(old, jnp.max(scores, axis=-1, keepdims=True))
    probs = [jnp.exp2((scores[:, t : t + 128] - new) * factor) for t in range(0, scores.shape[1], 128)]
    summed = jnp.dot(
        jnp.concatenate([p.astype(BF16) for p in probs], axis=1), values, preferred_element_type=F32
    )
    return new, jnp.exp2((old - new) * factor), sum(probs[1:], probs[0]), summed


def step_kernel(step, count, len_ref, q2_ref, f_ref, b_ref, unused_m, unused_l, unused_acc, m_ref, l_ref, acc_ref):
    i = lax.axis_index("seq")

    @pl.when(i >= step)
    def run():
        wrapped = i + step - count
        lengths = [
            len_ref[jnp.maximum(i - step, 0)],
            jnp.where(wrapped >= 0, len_ref[jnp.maximum(wrapped, 0)], 0),
        ]
        new, shrink, total, summed = attend(q2_ref, [f_ref, b_ref], lengths, m_ref)
        m_ref[...] = new
        l_ref[...] = shrink * l_ref[...] + total
        acc_ref[...] = shrink * acc_ref[...] + summed


def last_kernel(step, len_ref, q2_ref, f_ref, m_ref, l_ref, acc_ref, out_ref):
    i = lax.axis_index("seq")
    rows, width = f_ref.shape[0] // 2, f_ref.shape[1]
    heads = q2_ref.shape[0] // rows
    live = lax.broadcasted_iota(jnp.int32, (rows, 1), 0) < len_ref[i]

    def finish(total, summed):
        result = summed / jnp.sum(total, axis=-1, keepdims=True)
        for h in range(heads):
            picked = jnp.where(live, result[h * rows : (h + 1) * rows, :], 0.0)
            out_ref[:, h * width : (h + 1) * width] = picked.astype(BF16)

    @pl.when(i >= step)
    def run():
        _, shrink, total, summed = attend(q2_ref, [f_ref], [len_ref[jnp.maximum(i - step, 0)]], m_ref)
        finish(shrink * l_ref[...] + total, shrink * acc_ref[...] + summed)

    @pl.when(i < step)
    def skip():
        finish(l_ref[...], acc_ref[...])


def body(
    light_queries,
    light_keys,
    light_values,
    decay_log,
    norm_gain,
    soft_queries,
    soft_keys,
    soft_values,
    lengths,
):
    rows = light_queries.shape[0]
    heads = decay_log.shape[1]
    width = light_queries.shape[1] // heads
    count = lax.axis_size("seq")
    half = heads // 2
    back = count // 2 - 1

    def forward(step):
        return [(i, i + 1) for i in range(step - 1, count - 1)]

    def backward(step):
        return [((j + 1) % count, j) for j in range(count) if j + step < back or j + step >= count]

    def send(x, pairs):
        return lax.ppermute(x, "seq", pairs)

    def exchange(x, distance):
        return send(x, [(i, i ^ distance) for i in range(count)])

    lens = (True, lengths)
    own_kv = jnp.concatenate([soft_keys, soft_values], axis=0)
    f = send(own_kv, forward(1))
    b = send(own_kv, backward(1))

    msg, kept, logs, running, running_t = call(
        prep_kernel,
        [
            ((half * width + E_ROWS, width), BF16),
            ((half, width, width), F32),
            ((heads, 128), F32),
            ((heads, rows), F32),
            ((rows, heads), F32),
        ],
        [lens, (None, light_keys), (None, light_values), (False, decay_log.T)],
        scratch=[
            pltpu.VMEM((heads, width, width), F32),
            pltpu.VMEM((rows, heads * width), BF16),
            pltpu.VMEM((rows, heads * width), BF16),
            pltpu.SemaphoreType.DMA((2,)),
        ],
    )
    saved = []
    n = half
    for level in range(3):
        recv = exchange(msg, 1 << level)
        m = max(n // 2, 1)
        tail = E_ROWS if n > 1 else 0
        msg, nxt, low, low_logs, new_logs = call(
            partial(up_kernel, level),
            [
                ((m * width + tail, width), BF16),
                ((m, width, width), F32),
                ((n, width, width), F32),
                ((heads, 128), F32),
                ((heads, 128), F32),
            ],
            [(False, recv), (False, kept), (False, logs)],
        )
        saved.append((low, low_logs))
        kept, logs, n = (nxt, new_logs, n // 2)
    recv = send(msg, [(i, (i + 4 if i >= 4 else i - 4) % count) for i in range(count // 2)])
    held = None
    for level in (2, 1, 0):
        low, low_logs = saved[level]
        n = low.shape[0]
        ins = [(False, recv), (False, low), (False, low_logs)]
        if held is not None:
            ins = [(False, held)] + ins
        held, msg = call(
            partial(down_kernel, level, held is None), [((n, width, width), F32), ((n * width, width), BF16)], ins
        )
        recv = exchange(msg, 1 << level)
    (inside,) = call(
        inside_kernel,
        [((rows, heads * width), F32)],
        [
            lens,
            (False, light_queries),
            (False, light_keys),
            (False, light_values),
            (False, running),
            (False, running_t),
        ],
    )
    (light_out,) = call(
        light_kernel,
        [((rows, heads * width), BF16)],
        [
            lens,
            (False, light_queries),
            (False, inside),
            (False, held),
            (False, recv),
            (False, running_t),
            (False, norm_gain.reshape(1, heads * width)),
        ],
    )

    soft_rows = soft_queries.shape[1] // width * rows
    stat = ((soft_rows, 128), F32)
    q2, *state = call(
        own_kernel,
        [((soft_rows, width + 128), BF16), stat, stat, stat],
        [lens, (False, soft_queries), (False, soft_keys), (False, soft_values)],
    )
    for step in range(1, count // 2):
        nf = send(f, forward(step + 1))
        nb = send(b, backward(step + 1)) if step + 1 < count // 2 else None
        state = call(
            partial(step_kernel, step, count),
            [stat, stat, stat],
            [lens, (False, q2), (False, f), (False, b)] + [(False, s) for s in state],
            aliases={4: 0, 5: 1, 6: 2},
        )
        f, b = nf, nb
    (soft_out,) = call(
        partial(last_kernel, count // 2),
        [((rows, soft_queries.shape[1]), BF16)],
        [lens, (False, q2), (False, f)] + [(False, s) for s in state],
    )
    return (light_out, soft_out)


def solution(mesh):
    return jax.shard_map(
        body,
        mesh=mesh,
        in_specs=(
            P(("groups", "seq"), ("section", "mp")),
            P(("groups", "seq"), ("section", "mp")),
            P(("groups", "seq"), ("section", "mp")),
            P(("groups", "seq"), ("section", "mp")),
            P(("section", "mp")),
            P(("groups", "seq"), ("section", "mp")),
            P(("groups", "seq"), ("section", "mp")),
            P(("groups", "seq"), ("section", "mp")),
            P("groups"),
        ),
        out_specs=(
            P(("groups", "seq"), ("section", "mp")),
            P(("groups", "seq"), ("section", "mp")),
        ),
        check_vma=False,
    )
```

```python
from functools import partial

import jax
import jax.numpy as jnp
from jax import lax
from jax.experimental import pallas as pl
from jax.experimental.pallas import tpu as pltpu
from jax.sharding import PartitionSpec as P


F32 = jnp.float32
BF16 = jnp.bfloat16
NEG = -1e30
LOG2E = 1.4426950408889634
E_ROWS = 32
VMEM = pl.BlockSpec(memory_space=pltpu.VMEM)
ANY = pl.BlockSpec(memory_space=pltpu.HBM)


def call(kernel, out_shape, ins, aliases=None, flops=2_000_000, scratch=(), limit=48 * 1024 * 1024):
    specs = [ANY if s is None else VMEM for s, unused in ins]
    arrays = [a for unused, a in ins]
    outs = [jax.ShapeDtypeStruct(s, d) for s, d in out_shape]
    return pl.pallas_call(
        kernel,
        out_shape=outs,
        in_specs=specs,
        out_specs=[VMEM] * len(outs),
        scratch_shapes=list(scratch),
        input_output_aliases=aliases or {},
        compiler_params=pltpu.CompilerParams(vmem_limit_bytes=limit),
        cost_estimate=pl.CostEstimate(flops=flops, bytes_accessed=1 << 20, transcendentals=0),
    )(*arrays)


def bit(i, level):
    return lax.shift_right_logical(i, level) & 1


def keep_bit(i, level):
    return bit(i, level) ^ (bit(i, 3) if level == 2 else 0)


def first_head(i, level):
    start = keep_bit(i, 0) * 4
    if level >= 1:
        start += keep_bit(i, 1) * 2
    if level >= 2:
        start += keep_bit(i, 2)
    return start


def put_logs(msg_ref, at, logs):
    hi = logs.astype(BF16)
    rest = logs - hi.astype(F32)
    mid = rest.astype(BF16)
    low = (rest - mid.astype(F32)).astype(BF16)
    both = jnp.concatenate([hi.astype(F32), mid.astype(F32), low.astype(F32), jnp.zeros_like(logs)], axis=0)
    msg_ref[pl.ds(at, E_ROWS), :] = both.astype(BF16)


def get_logs(msg_ref, at):
    rows = msg_ref[pl.ds(at, E_ROWS), :].astype(F32)
    return rows[0:8] + rows[8:16] + rows[16:24]


def prep_kernel(
    len_ref, k_hbm, v_hbm, dec_ref, msg_ref, kept_ref, logs_ref, c_ref, ct_ref, bias_ref, live_ref, states, k_ref, v_ref, sems
):
    k_copy = pltpu.make_async_copy(k_hbm, k_ref, sems.at[0])
    v_copy = pltpu.make_async_copy(v_hbm, v_ref, sems.at[1])
    k_copy.start()
    v_copy.start()
    i = lax.axis_index("seq")
    rows = k_ref.shape[0]
    heads = dec_ref.shape[0]
    width = k_ref.shape[1] // heads
    half = heads // 2
    blocks = len_ref.shape[1]
    lengths = len_ref[...]
    at = lax.broadcasted_iota(jnp.int32, (1, blocks), 1)
    length = jnp.sum(jnp.where(at == i, lengths, 0), axis=1, keepdims=True)
    live_ref[...] = (lax.broadcasted_iota(jnp.int32, (rows, 128), 0) < length).astype(F32)
    square = (blocks, blocks)
    diagonal = lax.broadcasted_iota(jnp.int32, square, 0) == lax.broadcasted_iota(jnp.int32, square, 1)
    column = jnp.sum(jnp.where(diagonal, lengths, 0), axis=1, keepdims=True)
    dead = lax.broadcasted_iota(jnp.int32, (blocks, rows), 1) >= column
    bias_ref[0:blocks, :] = jnp.where(dead, NEG, 0.0)
    bias_ref[blocks:, :] = jnp.full((8, rows), NEG, F32)
    lane = lax.broadcasted_iota(jnp.int32, (heads, rows), 1)
    live = lane < length
    masked = jnp.where(live, dec_ref[...], 0.0)
    tri = (
        lax.broadcasted_iota(jnp.int32, (rows, rows), 0)
        <= lax.broadcasted_iota(jnp.int32, (rows, rows), 1)
    ).astype(F32)
    running = jnp.dot(masked, tri, preferred_element_type=F32, precision=lax.Precision.HIGHEST)
    ending = running[:, rows - 1 : rows]
    c_ref[...] = running
    ct_ref[...] = running.T
    logs = jnp.broadcast_to(ending, (heads, 128))
    logs_ref[...] = logs
    fading = jnp.where(live, jnp.exp(ending - running), 0.0)
    k_copy.wait()
    v_copy.wait()
    for h in range(heads):
        kt = k_ref[:, h * width : (h + 1) * width].T.astype(F32)
        scaled = (kt * fading[h : h + 1, :]).astype(BF16)
        states[h] = jnp.dot(scaled, v_ref[:, h * width : (h + 1) * width], preferred_element_type=F32)
    keep = keep_bit(i, 0) * half
    send = half - keep
    for h in range(half):
        kept_ref[h] = states[keep + h]
        msg_ref[h * width : (h + 1) * width, :] = states[send + h].astype(BF16)
    put_logs(msg_ref, half * width, logs)


def up_kernel(level, recv_ref, kept_ref, logs_ref, msg_ref, low_ref, lowlog_ref, next_ref=None, sum_ref=None):
    i = lax.axis_index("seq")
    count, width = kept_ref.shape[0], kept_ref.shape[1]
    upper = bit(i, level) == 1
    own = logs_ref[...]
    other = get_logs(recv_ref, count * width)
    low_logs = jnp.where(upper, other, own)
    lowlog_ref[...] = low_logs
    grown = jnp.exp(jnp.where(upper, own, other))
    start = first_head(i, level)
    which = lax.broadcasted_iota(jnp.int32, grown.shape, 0)
    half = count // 2
    keep = keep_bit(i, level + 1) * half
    totals = []
    for h in range(count):
        factor = jnp.sum(jnp.where(which == start + h, grown, 0.0), axis=0, keepdims=True)
        mine = kept_ref[h]
        got = recv_ref[h * width : (h + 1) * width, :].astype(F32)
        low = jnp.where(upper, got, mine)
        high = jnp.where(upper, mine, got)
        low_ref[h] = low
        totals.append(factor * low + high)
    if count == 1:
        msg_ref[...] = totals[0].astype(BF16)
        return
    sum_ref[...] = own + other
    first = keep == 0
    for h in range(half):
        next_ref[h] = jnp.where(first, totals[h], totals[half + h])
        msg_ref[h * width : (h + 1) * width, :] = jnp.where(first, totals[half + h], totals[h]).astype(BF16)
    put_logs(msg_ref, half * width, own + other)


def down_kernel(level, top, *refs):
    if top:
        recv_ref, low_ref, lowlog_ref, mine_ref, msg_ref = refs
    else:
        held_ref, recv_ref, low_ref, lowlog_ref, mine_ref, msg_ref = refs
    i = lax.axis_index("seq")
    count, width = low_ref.shape[0], low_ref.shape[1]
    half = count // 2
    upper = bit(i, level) == 1
    grown = jnp.exp(lowlog_ref[...])
    start = first_head(i, level)
    which = lax.broadcasted_iota(jnp.int32, grown.shape, 0)
    if top:
        entering = [recv_ref[...].astype(F32)]
    else:
        first = keep_bit(i, level + 1) == 0
        held = [held_ref[h] for h in range(half)]
        got = [recv_ref[h * width : (h + 1) * width, :].astype(F32) for h in range(half)]
        entering = [jnp.where(first, a, b) for a, b in zip(held, got)]
        entering += [jnp.where(first, b, a) for a, b in zip(held, got)]
    for h in range(count):
        factor = jnp.sum(jnp.where(which == start + h, grown, 0.0), axis=0, keepdims=True)
        low = entering[h]
        high = factor * low + low_ref[h]
        mine_ref[h] = jnp.where(upper, high, low)
        msg_ref[h * width : (h + 1) * width, :] = jnp.where(upper, low, high).astype(BF16)


def inside_kernel(bias_ref, q_ref, k_ref, v_ref, c_ref, ct_ref, out_ref):
    i = lax.axis_index("seq")
    rows = q_ref.shape[0]
    heads = c_ref.shape[0]
    width = q_ref.shape[1] // heads
    scale = width ** (-0.5)
    row = lax.broadcasted_iota(jnp.int32, (rows, rows), 0)
    col = lax.broadcasted_iota(jnp.int32, (rows, rows), 1)
    allowed = (col <= row) & (bias_ref[pl.ds(i, 1), :] == 0.0)
    running = c_ref[...]
    running_t = ct_ref[...]
    for h in range(heads):
        at = slice(h * width, (h + 1) * width)
        scores = lax.dot_general(
            q_ref[:, at], k_ref[:, at], (((1,), (1,)), ((), ())), preferred_element_type=F32
        )
        gaps = running_t[:, h : h + 1] - running[h : h + 1, :]
        weights = jnp.exp(jnp.where(allowed, gaps, NEG))
        intra = (scores * scale * weights).astype(BF16)
        out_ref[:, at] = jnp.dot(intra, v_ref[:, at], preferred_element_type=F32)


def light_kernel(live_ref, q_ref, inside_ref, held_ref, recv_ref, ct_ref, gain_ref, out_ref):
    i = lax.axis_index("seq")
    half, width = held_ref.shape[0], held_ref.shape[1]
    scale = width ** (-0.5)
    first = keep_bit(i, 0) == 0
    live = live_ref[...] > 0.0
    grown = jnp.exp(ct_ref[...]) * scale
    for h in range(2 * half):
        at = slice(h * width, (h + 1) * width)
        mod = h % half
        held = held_ref[mod].astype(BF16)
        got = recv_ref[mod * width : (mod + 1) * width, :]
        pick_held = first if h < half else jnp.logical_not(first)
        entering = jnp.where(pick_held, held.astype(F32), got.astype(F32)).astype(BF16)
        across = jnp.dot(q_ref[:, at], entering, preferred_element_type=F32)
        combined = inside_ref[:, at] + across * grown[:, h : h + 1]
        mean = jnp.mean(combined * combined, axis=-1, keepdims=True)
        normed = combined * lax.rsqrt(mean + 1e-06) * gain_ref[:, at]
        out_ref[:, at] = jnp.where(live, normed, 0.0).astype(BF16)


def unit_columns(rows):
    return jnp.where(lax.broadcasted_iota(jnp.int32, (rows, 128), 1) == 0, 1.0, 0.0).astype(BF16)


def own_kernel(bias_ref, q_ref, k_ref, v_ref, q2_ref, m_ref, l_ref, acc_ref):
    i = lax.axis_index("seq")
    rows, width = k_ref.shape
    heads = q_ref.shape[1] // width
    factor = width ** (-0.5) * LOG2E
    q2_ref[:, width:] = unit_columns(heads * rows)
    for h in range(heads):
        q2_ref[h * rows : (h + 1) * rows, :width] = q_ref[:, h * width : (h + 1) * width]
    row = lax.broadcasted_iota(jnp.int32, (rows, rows), 0)
    col = lax.broadcasted_iota(jnp.int32, (rows, rows), 1)
    allowed = (col <= row) & (bias_ref[pl.ds(i, 1), :] == 0.0)
    scores = jnp.dot(q2_ref[:, :width], k_ref[...].T, preferred_element_type=F32)
    scores = jnp.where(allowed[None], scores.reshape(heads, rows, rows), NEG).reshape(heads * rows, rows)
    peak = jnp.broadcast_to(jnp.max(scores, axis=-1, keepdims=True), (heads * rows, 128))
    probs = [jnp.exp2((scores[:, t : t + 128] - peak) * factor) for t in range(0, rows, 128)]
    m_ref[...] = peak
    l_ref[...] = sum(probs[1:], probs[0])
    acc_ref[...] = jnp.dot(
        jnp.concatenate([p.astype(BF16) for p in probs], axis=1), v_ref[...], preferred_element_type=F32
    )


def attend(q2_ref, blocks, biases, old_ref):
    rows, width = blocks[0].shape[0] // 2, blocks[0].shape[1]
    factor = width ** (-0.5) * LOG2E
    row = lax.broadcasted_iota(jnp.int32, (128, rows), 0)
    biases = [jnp.where(row == 0, bias, 0.0).astype(BF16) for bias in biases]
    keys_t = jnp.concatenate([ref[0:rows, :].T for ref in blocks], axis=1)
    keys_t = jnp.concatenate([keys_t, jnp.concatenate(biases, axis=1)], axis=0)
    values = jnp.concatenate([ref[rows : 2 * rows, :] for ref in blocks], axis=0)
    scores = jnp.dot(q2_ref[...], keys_t, preferred_element_type=F32)
    old = old_ref[...]
    new = jnp.maximum(old, jnp.max(scores, axis=-1, keepdims=True))
    probs = [jnp.exp2((scores[:, t : t + 128] - new) * factor) for t in range(0, scores.shape[1], 128)]
    summed = jnp.dot(
        jnp.concatenate([p.astype(BF16) for p in probs], axis=1), values, preferred_element_type=F32
    )
    return new, jnp.exp2((old - new) * factor), sum(probs[1:], probs[0]), summed


def step_kernel(step, count, bias_ref, q2_ref, f_ref, b_ref, unused_m, unused_l, unused_acc, m_ref, l_ref, acc_ref):
    i = lax.axis_index("seq")

    @pl.when(i >= step)
    def run():
        wrapped = i + step - count
        biases = [
            bias_ref[pl.ds(i - step, 1), :],
            bias_ref[pl.ds(jnp.where(wrapped >= 0, wrapped, count), 1), :],
        ]
        new, shrink, total, summed = attend(q2_ref, [f_ref, b_ref], biases, m_ref)
        m_ref[...] = new
        l_ref[...] = shrink * l_ref[...] + total
        acc_ref[...] = shrink * acc_ref[...] + summed


def last_kernel(step, bias_ref, live_ref, q2_ref, f_ref, m_ref, l_ref, acc_ref, out_ref):
    i = lax.axis_index("seq")
    rows, width = f_ref.shape[0] // 2, f_ref.shape[1]
    heads = q2_ref.shape[0] // rows
    live = live_ref[...] > 0.0

    def finish(total, summed):
        result = summed / jnp.sum(total, axis=-1, keepdims=True)
        for h in range(heads):
            picked = jnp.where(live, result[h * rows : (h + 1) * rows, :], 0.0)
            out_ref[:, h * width : (h + 1) * width] = picked.astype(BF16)

    @pl.when(i >= step)
    def run():
        _, shrink, total, summed = attend(q2_ref, [f_ref], [bias_ref[pl.ds(i - step, 1), :]], m_ref)
        finish(shrink * l_ref[...] + total, shrink * acc_ref[...] + summed)

    @pl.when(i < step)
    def skip():
        finish(l_ref[...], acc_ref[...])


def body(
    light_queries,
    light_keys,
    light_values,
    decay_log,
    norm_gain,
    soft_queries,
    soft_keys,
    soft_values,
    lengths,
):
    rows = light_queries.shape[0]
    heads = decay_log.shape[1]
    width = light_queries.shape[1] // heads
    count = lax.axis_size("seq")
    half = heads // 2

    def forward():
        return [(i, (i + 1) % count) for i in range(count)]

    def backward():
        return [((j + 1) % count, j) for j in range(count)]

    def send(x, pairs):
        return lax.ppermute(x, "seq", pairs)

    def exchange(x, distance):
        return send(x, [(i, i ^ distance) for i in range(count)])

    own_kv = jnp.concatenate([soft_keys, soft_values], axis=0)
    f = send(own_kv, forward())
    b = send(own_kv, backward())

    msg, kept, logs, running, running_t, bias, live = call(
        prep_kernel,
        [
            ((half * width + E_ROWS, width), BF16),
            ((half, width, width), F32),
            ((heads, 128), F32),
            ((heads, rows), F32),
            ((rows, heads), F32),
            ((count + 8, rows), F32),
            ((rows, 128), F32),
        ],
        [(False, lengths.reshape(1, count)), (None, pltpu.with_memory_space_constraint(light_keys, pltpu.HBM)), (None, pltpu.with_memory_space_constraint(light_values, pltpu.HBM)), (False, decay_log.T)],
        scratch=[
            pltpu.VMEM((heads, width, width), F32),
            pltpu.VMEM((rows, heads * width), BF16),
            pltpu.VMEM((rows, heads * width), BF16),
            pltpu.SemaphoreType.DMA((2,)),
        ],
        limit=48 * 1024 * 1024,
    )
    saved = []
    n = half
    for level in range(3):
        recv = exchange(msg, 1 << level)
        m = max(n // 2, 1)
        tail = E_ROWS if n > 1 else 0
        onward = [((m, width, width), F32), ((heads, 128), F32)] if n > 1 else []
        msg, low, low_logs, *rest = call(
            partial(up_kernel, level),
            [((m * width + tail, width), BF16), ((n, width, width), F32), ((heads, 128), F32)] + onward,
            [(False, recv), (False, kept), (False, logs)],
        )
        saved.append((low, low_logs))
        n //= 2
        if n:
            kept, logs = rest
    recv = send(msg, [(i, (i + 4 if i >= 4 else i - 4) % count) for i in range(count // 2)])
    held = None
    for level in (2, 1, 0):
        low, low_logs = saved[level]
        n = low.shape[0]
        ins = [(False, recv), (False, low), (False, low_logs)]
        if held is not None:
            ins = [(False, held)] + ins
        held, msg = call(
            partial(down_kernel, level, held is None), [((n, width, width), F32), ((n * width, width), BF16)], ins
        )
        recv = exchange(msg, 1 << level)
    (inside,) = call(
        inside_kernel,
        [((rows, heads * width), F32)],
        [
            (False, bias),
            (False, light_queries),
            (False, light_keys),
            (False, light_values),
            (False, running),
            (False, running_t),
        ],
    )
    (light_out,) = call(
        light_kernel,
        [((rows, heads * width), BF16)],
        [
            (False, live),
            (False, light_queries),
            (False, inside),
            (False, held),
            (False, recv),
            (False, running_t),
            (False, norm_gain.reshape(1, heads * width)),
        ],
    )

    soft_rows = soft_queries.shape[1] // width * rows
    stat = ((soft_rows, 128), F32)
    q2, *state = call(
        own_kernel,
        [((soft_rows, width + 128), BF16), stat, stat, stat],
        [(False, bias), (False, soft_queries), (False, soft_keys), (False, soft_values)],
    )
    for step in range(1, count // 2):
        nf = send(f, forward())
        nb = send(b, backward()) if step + 1 < count // 2 else None
        state = call(
            partial(step_kernel, step, count),
            [stat, stat, stat],
            [(False, bias), (False, q2), (False, f), (False, b)] + [(False, s) for s in state],
            aliases={4: 0, 5: 1, 6: 2},
        )
        f, b = nf, nb
    (soft_out,) = call(
        partial(last_kernel, count // 2),
        [((rows, soft_queries.shape[1]), BF16)],
        [(False, bias), (False, live), (False, q2), (False, f)] + [(False, s) for s in state],
    )
    return (light_out, soft_out)


def solution(mesh):
    return jax.shard_map(
        body,
        mesh=mesh,
        in_specs=(
            P(("groups", "seq"), ("section", "mp")),
            P(("groups", "seq"), ("section", "mp")),
            P(("groups", "seq"), ("section", "mp")),
            P(("groups", "seq"), ("section", "mp")),
            P(("section", "mp")),
            P(("groups", "seq"), ("section", "mp")),
            P(("groups", "seq"), ("section", "mp")),
            P(("groups", "seq"), ("section", "mp")),
            P("groups"),
        ),
        out_specs=(
            P(("groups", "seq"), ("section", "mp")),
            P(("groups", "seq"), ("section", "mp")),
        ),
        check_vma=False,
    )
```

```python
from functools import partial

import jax
import jax.numpy as jnp
from jax import lax
from jax.experimental import pallas as pl
from jax.experimental.pallas import tpu as pltpu
from jax.sharding import PartitionSpec as P


F32 = jnp.float32
BF16 = jnp.bfloat16
NEG = -1e30
LOG2E = 1.4426950408889634
E_ROWS = 32
VMEM = pl.BlockSpec(memory_space=pltpu.VMEM)
ANY = pl.BlockSpec(memory_space=pltpu.HBM)


def call(kernel, out_shape, ins, aliases=None, flops=2_000_000, scratch=(), limit=48 * 1024 * 1024):
    specs = [ANY if s is None else VMEM for s, unused in ins]
    arrays = [a for unused, a in ins]
    outs = [jax.ShapeDtypeStruct(s, d) for s, d in out_shape]
    return pl.pallas_call(
        kernel,
        out_shape=outs,
        in_specs=specs,
        out_specs=[VMEM] * len(outs),
        scratch_shapes=list(scratch),
        input_output_aliases=aliases or {},
        compiler_params=pltpu.CompilerParams(vmem_limit_bytes=limit),
        cost_estimate=pl.CostEstimate(flops=flops, bytes_accessed=1 << 20, transcendentals=0),
    )(*arrays)


def bit(i, level):
    return lax.shift_right_logical(i, level) & 1


def keep_bit(i, level):
    return bit(i, level) ^ (bit(i, 3) if level == 2 else 0)


def first_head(i, level):
    start = keep_bit(i, 0) * 4
    if level >= 1:
        start += keep_bit(i, 1) * 2
    if level >= 2:
        start += keep_bit(i, 2)
    return start


def put_logs(msg_ref, at, logs):
    hi = logs.astype(BF16)
    rest = logs - hi.astype(F32)
    mid = rest.astype(BF16)
    low = (rest - mid.astype(F32)).astype(BF16)
    both = jnp.concatenate([hi.astype(F32), mid.astype(F32), low.astype(F32), jnp.zeros_like(logs)], axis=0)
    msg_ref[pl.ds(at, E_ROWS), :] = both.astype(BF16)


def get_logs(msg_ref, at):
    rows = msg_ref[pl.ds(at, E_ROWS), :].astype(F32)
    return rows[0:8] + rows[8:16] + rows[16:24]


def prep_kernel(
    len_ref, k_hbm, v_hbm, dec_ref, msg_ref, kept_ref, logs_ref, c_ref, ct_ref, bias_ref, live_ref, states, k_ref, v_ref, sems
):
    k_copy = pltpu.make_async_copy(k_hbm, k_ref, sems.at[0])
    v_copy = pltpu.make_async_copy(v_hbm, v_ref, sems.at[1])
    k_copy.start()
    v_copy.start()
    i = lax.axis_index("seq")
    rows = k_ref.shape[0]
    heads = dec_ref.shape[0]
    width = k_ref.shape[1] // heads
    half = heads // 2
    blocks = len_ref.shape[1]
    lengths = len_ref[...]
    at = lax.broadcasted_iota(jnp.int32, (1, blocks), 1)
    length = jnp.sum(jnp.where(at == i, lengths, 0), axis=1, keepdims=True)
    live_ref[...] = (lax.broadcasted_iota(jnp.int32, (rows, 128), 0) < length).astype(F32)
    square = (blocks, blocks)
    diagonal = lax.broadcasted_iota(jnp.int32, square, 0) == lax.broadcasted_iota(jnp.int32, square, 1)
    column = jnp.sum(jnp.where(diagonal, lengths, 0), axis=1, keepdims=True)
    dead = lax.broadcasted_iota(jnp.int32, (blocks, rows), 1) >= column
    bias_ref[0:blocks, :] = jnp.where(dead, NEG, 0.0)
    bias_ref[blocks:, :] = jnp.full((8, rows), NEG, F32)
    lane = lax.broadcasted_iota(jnp.int32, (heads, rows), 1)
    live = lane < length
    masked = jnp.where(live, dec_ref[...], 0.0)
    tri = (
        lax.broadcasted_iota(jnp.int32, (rows, rows), 0)
        <= lax.broadcasted_iota(jnp.int32, (rows, rows), 1)
    ).astype(F32)
    running = jnp.dot(masked, tri, preferred_element_type=F32, precision=lax.Precision.HIGHEST)
    ending = running[:, rows - 1 : rows]
    c_ref[...] = running
    ct_ref[...] = running.T
    logs = jnp.broadcast_to(ending, (heads, 128))
    logs_ref[...] = logs
    fading = jnp.where(live, jnp.exp(ending - running), 0.0)
    k_copy.wait()
    v_copy.wait()
    for h in range(heads):
        kt = k_ref[:, h * width : (h + 1) * width].T.astype(F32)
        scaled = (kt * fading[h : h + 1, :]).astype(BF16)
        states[h] = jnp.dot(scaled, v_ref[:, h * width : (h + 1) * width], preferred_element_type=F32)
    keep = keep_bit(i, 0) * half
    send = half - keep
    for h in range(half):
        kept_ref[h] = states[keep + h]
        msg_ref[h * width : (h + 1) * width, :] = states[send + h].astype(BF16)
    put_logs(msg_ref, half * width, logs)


def up_kernel(level, recv_ref, kept_ref, logs_ref, msg_ref, low_ref, lowlog_ref, next_ref=None, sum_ref=None):
    i = lax.axis_index("seq")
    count, width = kept_ref.shape[0], kept_ref.shape[1]
    upper = bit(i, level) == 1
    own = logs_ref[...]
    other = get_logs(recv_ref, count * width)
    low_logs = jnp.where(upper, other, own)
    lowlog_ref[...] = low_logs
    grown = jnp.exp(jnp.where(upper, own, other))
    start = first_head(i, level)
    which = lax.broadcasted_iota(jnp.int32, grown.shape, 0)
    half = count // 2
    keep = keep_bit(i, level + 1) * half
    totals = []
    for h in range(count):
        factor = jnp.sum(jnp.where(which == start + h, grown, 0.0), axis=0, keepdims=True)
        mine = kept_ref[h]
        got = recv_ref[h * width : (h + 1) * width, :].astype(F32)
        low = jnp.where(upper, got, mine)
        high = jnp.where(upper, mine, got)
        low_ref[h] = low
        totals.append(factor * low + high)
    if count == 1:
        msg_ref[...] = totals[0].astype(BF16)
        return
    sum_ref[...] = own + other
    first = keep == 0
    for h in range(half):
        next_ref[h] = jnp.where(first, totals[h], totals[half + h])
        msg_ref[h * width : (h + 1) * width, :] = jnp.where(first, totals[half + h], totals[h]).astype(BF16)
    put_logs(msg_ref, half * width, own + other)


def down_kernel(level, top, *refs):
    if top:
        recv_ref, low_ref, lowlog_ref, mine_ref, msg_ref = refs
    else:
        held_ref, recv_ref, low_ref, lowlog_ref, mine_ref, msg_ref = refs
    i = lax.axis_index("seq")
    count, width = low_ref.shape[0], low_ref.shape[1]
    half = count // 2
    upper = bit(i, level) == 1
    grown = jnp.exp(lowlog_ref[...])
    start = first_head(i, level)
    which = lax.broadcasted_iota(jnp.int32, grown.shape, 0)
    if top:
        entering = [recv_ref[...].astype(F32)]
    else:
        first = keep_bit(i, level + 1) == 0
        held = [held_ref[h] for h in range(half)]
        got = [recv_ref[h * width : (h + 1) * width, :].astype(F32) for h in range(half)]
        entering = [jnp.where(first, a, b) for a, b in zip(held, got)]
        entering += [jnp.where(first, b, a) for a, b in zip(held, got)]
    for h in range(count):
        factor = jnp.sum(jnp.where(which == start + h, grown, 0.0), axis=0, keepdims=True)
        low = entering[h]
        high = factor * low + low_ref[h]
        mine_ref[h] = jnp.where(upper, high, low)
        msg_ref[h * width : (h + 1) * width, :] = jnp.where(upper, low, high).astype(BF16)


def inside_kernel(bias_ref, q_ref, k_ref, v_ref, c_ref, ct_ref, gain_ref, out_ref, scaled_ref, gain_out_ref):
    gain_out_ref[...] = gain_ref[...]
    i = lax.axis_index("seq")
    rows = q_ref.shape[0]
    heads = c_ref.shape[0]
    width = q_ref.shape[1] // heads
    scale = width ** (-0.5)
    row = lax.broadcasted_iota(jnp.int32, (rows, rows), 0)
    col = lax.broadcasted_iota(jnp.int32, (rows, rows), 1)
    allowed = (col <= row) & (bias_ref[pl.ds(i, 1), :] == 0.0)
    running = c_ref[...]
    running_t = ct_ref[...]
    grown = jnp.exp(running_t) * scale
    for h in range(heads):
        at = slice(h * width, (h + 1) * width)
        scores = lax.dot_general(
            q_ref[:, at], k_ref[:, at], (((1,), (1,)), ((), ())), preferred_element_type=F32
        )
        scaled_ref[:, at] = (q_ref[:, at].astype(F32) * grown[:, h : h + 1]).astype(BF16)
        gaps = running_t[:, h : h + 1] - running[h : h + 1, :]
        weights = jnp.exp(jnp.where(allowed, gaps, NEG))
        intra = (scores * scale * weights).astype(BF16)
        out_ref[:, at] = jnp.dot(intra, v_ref[:, at], preferred_element_type=F32)


def light_kernel(live_ref, q_ref, inside_ref, held_ref, recv_ref, gain_ref, out_ref):
    i = lax.axis_index("seq")
    half, width = held_ref.shape[0], held_ref.shape[1]
    first = keep_bit(i, 0) == 0
    live = live_ref[...] > 0.0
    for h in range(2 * half):
        at = slice(h * width, (h + 1) * width)
        mod = h % half
        held = held_ref[mod].astype(BF16)
        got = recv_ref[mod * width : (mod + 1) * width, :]
        pick_held = first if h < half else jnp.logical_not(first)
        entering = jnp.where(pick_held, held.astype(F32), got.astype(F32)).astype(BF16)
        across = jnp.dot(q_ref[:, at], entering, preferred_element_type=F32)
        combined = inside_ref[:, at] + across
        mean = jnp.mean(combined * combined, axis=-1, keepdims=True)
        normed = combined * lax.rsqrt(mean + 1e-06) * gain_ref[:, at]
        out_ref[:, at] = jnp.where(live, normed, 0.0).astype(BF16)


def unit_columns(rows):
    return jnp.where(lax.broadcasted_iota(jnp.int32, (rows, 128), 1) == 0, 1.0, 0.0).astype(BF16)


def own_kernel(bias_ref, q_ref, k_ref, v_ref, q2_ref, m_ref, l_ref, acc_ref):
    i = lax.axis_index("seq")
    rows, width = k_ref.shape
    heads = q_ref.shape[1] // width
    factor = width ** (-0.5) * LOG2E
    q2_ref[:, width:] = unit_columns(heads * rows)
    for h in range(heads):
        q2_ref[h * rows : (h + 1) * rows, :width] = q_ref[:, h * width : (h + 1) * width]
    row = lax.broadcasted_iota(jnp.int32, (rows, rows), 0)
    col = lax.broadcasted_iota(jnp.int32, (rows, rows), 1)
    allowed = (col <= row) & (bias_ref[pl.ds(i, 1), :] == 0.0)
    scores = jnp.dot(q2_ref[:, :width], k_ref[...].T, preferred_element_type=F32)
    scores = jnp.where(allowed[None], scores.reshape(heads, rows, rows), NEG).reshape(heads * rows, rows)
    peak = jnp.broadcast_to(jnp.max(scores, axis=-1, keepdims=True), (heads * rows, 128))
    probs = [jnp.exp2((scores[:, t : t + 128] - peak) * factor) for t in range(0, rows, 128)]
    m_ref[...] = peak
    l_ref[...] = sum(probs[1:], probs[0])
    acc_ref[...] = jnp.dot(
        jnp.concatenate([p.astype(BF16) for p in probs], axis=1), v_ref[...], preferred_element_type=F32
    )


def attend(q2_ref, blocks, biases, old_ref):
    rows, width = blocks[0].shape[0] // 2, blocks[0].shape[1]
    factor = width ** (-0.5) * LOG2E
    row = lax.broadcasted_iota(jnp.int32, (128, rows), 0)
    biases = [jnp.where(row == 0, bias, 0.0).astype(BF16) for bias in biases]
    keys_t = jnp.concatenate([ref[0:rows, :].T for ref in blocks], axis=1)
    keys_t = jnp.concatenate([keys_t, jnp.concatenate(biases, axis=1)], axis=0)
    values = jnp.concatenate([ref[rows : 2 * rows, :] for ref in blocks], axis=0)
    scores = jnp.dot(q2_ref[...], keys_t, preferred_element_type=F32)
    old = old_ref[...]
    new = jnp.maximum(old, jnp.max(scores, axis=-1, keepdims=True))
    probs = [jnp.exp2((scores[:, t : t + 128] - new) * factor) for t in range(0, scores.shape[1], 128)]
    summed = jnp.dot(
        jnp.concatenate([p.astype(BF16) for p in probs], axis=1), values, preferred_element_type=F32
    )
    return new, jnp.exp2((old - new) * factor), sum(probs[1:], probs[0]), summed


def step_kernel(step, count, blocks, bias_ref, q2_ref, *refs):
    kv_refs, (m_ref, l_ref, acc_ref) = refs[:blocks], refs[-3:]
    i = lax.axis_index("seq")

    @pl.when(i >= step)
    def run():
        wrapped = i + step - count
        biases = [bias_ref[pl.ds(i - step, 1), :]]
        if blocks > 1:
            biases.append(bias_ref[pl.ds(jnp.where(wrapped >= 0, wrapped, count), 1), :])
        new, shrink, total, summed = attend(q2_ref, kv_refs, biases, m_ref)
        m_ref[...] = new
        l_ref[...] = shrink * l_ref[...] + total
        acc_ref[...] = shrink * acc_ref[...] + summed


def last_kernel(step, bias_ref, live_ref, q2_ref, f_ref, m_ref, l_ref, acc_ref, out_ref):
    i = lax.axis_index("seq")
    rows, width = f_ref.shape[0] // 2, f_ref.shape[1]
    heads = q2_ref.shape[0] // rows
    live = live_ref[...] > 0.0

    def finish(total, summed):
        result = summed / jnp.sum(total, axis=-1, keepdims=True)
        for h in range(heads):
            picked = jnp.where(live, result[h * rows : (h + 1) * rows, :], 0.0)
            out_ref[:, h * width : (h + 1) * width] = picked.astype(BF16)

    @pl.when(i >= step)
    def run():
        _, shrink, total, summed = attend(q2_ref, [f_ref], [bias_ref[pl.ds(i - step, 1), :]], m_ref)
        finish(shrink * l_ref[...] + total, shrink * acc_ref[...] + summed)

    @pl.when(i < step)
    def skip():
        finish(l_ref[...], acc_ref[...])


def body(
    light_queries,
    light_keys,
    light_values,
    decay_log,
    norm_gain,
    soft_queries,
    soft_keys,
    soft_values,
    lengths,
):
    rows = light_queries.shape[0]
    heads = decay_log.shape[1]
    width = light_queries.shape[1] // heads
    count = lax.axis_size("seq")
    half = heads // 2
    steps = count // 2
    backs = count - 1 - steps

    def forward(step):
        if step <= backs:
            return [(i, (i + 1) % count) for i in range(count)]
        return [(i, i + 1) for i in range(step - 1, count - 1)]

    backward = [((j + 1) % count, j) for j in range(count)]

    def send(x, pairs):
        return lax.ppermute(x, "seq", pairs)

    def exchange(x, distance):
        return send(x, [(i, i ^ distance) for i in range(count)])

    own_kv = jnp.concatenate([soft_keys, soft_values], axis=0)
    f = send(own_kv, forward(1))
    b = send(own_kv, backward)

    msg, kept, logs, running, running_t, bias, live = call(
        prep_kernel,
        [
            ((half * width + E_ROWS, width), BF16),
            ((half, width, width), F32),
            ((heads, 128), F32),
            ((heads, rows), F32),
            ((rows, heads), F32),
            ((count + 8, rows), F32),
            ((rows, 128), F32),
        ],
        [(False, lengths.reshape(1, count)), (None, pltpu.with_memory_space_constraint(light_keys, pltpu.HBM)), (None, pltpu.with_memory_space_constraint(light_values, pltpu.HBM)), (False, decay_log.T)],
        scratch=[
            pltpu.VMEM((heads, width, width), F32),
            pltpu.VMEM((rows, heads * width), BF16),
            pltpu.VMEM((rows, heads * width), BF16),
            pltpu.SemaphoreType.DMA((2,)),
        ],
        limit=48 * 1024 * 1024,
    )
    saved = []
    n = half
    for level in range(3):
        recv = exchange(msg, 1 << level)
        m = max(n // 2, 1)
        tail = E_ROWS if n > 1 else 0
        onward = [((m, width, width), F32), ((heads, 128), F32)] if n > 1 else []
        msg, low, low_logs, *rest = call(
            partial(up_kernel, level),
            [((m * width + tail, width), BF16), ((n, width, width), F32), ((heads, 128), F32)] + onward,
            [(False, recv), (False, kept), (False, logs)],
        )
        saved.append((low, low_logs))
        n //= 2
        if n:
            kept, logs = rest
    recv = send(msg, [(i, (i + 4 if i >= 4 else i - 4) % count) for i in range(count // 2)])
    held = None
    for level in (2, 1, 0):
        low, low_logs = saved[level]
        n = low.shape[0]
        ins = [(False, recv), (False, low), (False, low_logs)]
        if held is not None:
            ins = [(False, held)] + ins
        held, msg = call(
            partial(down_kernel, level, held is None), [((n, width, width), F32), ((n * width, width), BF16)], ins
        )
        recv = exchange(msg, 1 << level)
    inside, scaled, gain = call(
        inside_kernel,
        [((rows, heads * width), F32), ((rows, heads * width), BF16), ((1, heads * width), F32)],
        [
            (False, bias),
            (False, light_queries),
            (False, light_keys),
            (False, light_values),
            (False, running),
            (False, running_t),
            (False, norm_gain.reshape(1, heads * width)),
        ],
    )
    (light_out,) = call(
        light_kernel,
        [((rows, heads * width), BF16)],
        [
            (False, live),
            (False, scaled),
            (False, inside),
            (False, held),
            (False, recv),
            (False, gain),
        ],
    )

    soft_rows = soft_queries.shape[1] // width * rows
    stat = ((soft_rows, 128), F32)
    q2, *state = call(
        own_kernel,
        [((soft_rows, width + 128), BF16), stat, stat, stat],
        [(False, bias), (False, soft_queries), (False, soft_keys), (False, soft_values)],
    )
    for step in range(1, steps):
        nf = send(f, forward(step + 1))
        nb = send(b, backward) if step < backs else None
        blocks = [(False, f)] + ([(False, b)] if step <= backs else [])
        at = 2 + len(blocks)
        state = call(
            partial(step_kernel, step, count, len(blocks)),
            [stat, stat, stat],
            [(False, bias), (False, q2)] + blocks + [(False, s) for s in state],
            aliases={at: 0, at + 1: 1, at + 2: 2},
        )
        f, b = nf, nb
    (soft_out,) = call(
        partial(last_kernel, steps),
        [((rows, soft_queries.shape[1]), BF16)],
        [(False, bias), (False, live), (False, q2), (False, f)] + [(False, s) for s in state],
    )
    return (light_out, soft_out)


def solution(mesh):
    return jax.shard_map(
        body,
        mesh=mesh,
        in_specs=(
            P(("groups", "seq"), ("section", "mp")),
            P(("groups", "seq"), ("section", "mp")),
            P(("groups", "seq"), ("section", "mp")),
            P(("groups", "seq"), ("section", "mp")),
            P(("section", "mp")),
            P(("groups", "seq"), ("section", "mp")),
            P(("groups", "seq"), ("section", "mp")),
            P(("groups", "seq"), ("section", "mp")),
            P("groups"),
        ),
        out_specs=(
            P(("groups", "seq"), ("section", "mp")),
            P(("groups", "seq"), ("section", "mp")),
        ),
        check_vma=False,
    )
```

```python
from functools import partial

import jax
import jax.numpy as jnp
from jax import lax
from jax.experimental import pallas as pl
from jax.experimental.pallas import tpu as pltpu
from jax.sharding import PartitionSpec as P


F32 = jnp.float32
BF16 = jnp.bfloat16
NEG = -1e30
LOG2E = 1.4426950408889634
E_ROWS = 32
VMEM = pl.BlockSpec(memory_space=pltpu.VMEM)
ANY = pl.BlockSpec(memory_space=pltpu.HBM)


def call(kernel, out_shape, ins, aliases=None, flops=2_000_000, scratch=(), limit=48 * 1024 * 1024):
    specs = [ANY if s is None else VMEM for s, unused in ins]
    arrays = [a for unused, a in ins]
    outs = [jax.ShapeDtypeStruct(s, d) for s, d in out_shape]
    return pl.pallas_call(
        kernel,
        out_shape=outs,
        in_specs=specs,
        out_specs=[VMEM] * len(outs),
        scratch_shapes=list(scratch),
        input_output_aliases=aliases or {},
        compiler_params=pltpu.CompilerParams(vmem_limit_bytes=limit),
        cost_estimate=pl.CostEstimate(flops=flops, bytes_accessed=1 << 20, transcendentals=0),
    )(*arrays)


def bit(i, level):
    return lax.shift_right_logical(i, level) & 1


def first_head(i, level):
    start = bit(i, 0) * 4
    if level >= 1:
        start += bit(i, 1) * 2
    return start


def put_logs(msg_ref, at, logs):
    hi = logs.astype(BF16)
    rest = logs - hi.astype(F32)
    mid = rest.astype(BF16)
    low = (rest - mid.astype(F32)).astype(BF16)
    both = jnp.concatenate([hi.astype(F32), mid.astype(F32), low.astype(F32), jnp.zeros_like(logs)], axis=0)
    msg_ref[pl.ds(at, E_ROWS), :] = both.astype(BF16)


def get_logs(msg_ref, at):
    rows = msg_ref[pl.ds(at, E_ROWS), :].astype(F32)
    return rows[0:8] + rows[8:16] + rows[16:24]


def prep_kernel(
    len_ref, k_hbm, v_hbm, dec_ref, msg_ref, kept_ref, logs_ref, c_ref, ct_ref, bias_ref, live_ref, states, k_ref, v_ref, sems
):
    k_copy = pltpu.make_async_copy(k_hbm, k_ref, sems.at[0])
    v_copy = pltpu.make_async_copy(v_hbm, v_ref, sems.at[1])
    k_copy.start()
    v_copy.start()
    i = lax.axis_index("seq")
    rows = k_ref.shape[0]
    heads = dec_ref.shape[0]
    width = k_ref.shape[1] // heads
    half = heads // 2
    blocks = len_ref.shape[1]
    lengths = len_ref[...]
    at = lax.broadcasted_iota(jnp.int32, (1, blocks), 1)
    length = jnp.sum(jnp.where(at == i, lengths, 0), axis=1, keepdims=True)
    live_ref[...] = (lax.broadcasted_iota(jnp.int32, (rows, 128), 0) < length).astype(F32)
    square = (blocks, blocks)
    diagonal = lax.broadcasted_iota(jnp.int32, square, 0) == lax.broadcasted_iota(jnp.int32, square, 1)
    column = jnp.sum(jnp.where(diagonal, lengths, 0), axis=1, keepdims=True)
    dead = lax.broadcasted_iota(jnp.int32, (blocks, rows), 1) >= column
    bias_ref[0:blocks, :] = jnp.where(dead, NEG, 0.0)
    bias_ref[blocks:, :] = jnp.full((8, rows), NEG, F32)
    lane = lax.broadcasted_iota(jnp.int32, (heads, rows), 1)
    live = lane < length
    masked = jnp.where(live, dec_ref[...], 0.0)
    tri = (
        lax.broadcasted_iota(jnp.int32, (rows, rows), 0)
        <= lax.broadcasted_iota(jnp.int32, (rows, rows), 1)
    ).astype(F32)
    running = jnp.dot(masked, tri, preferred_element_type=F32, precision=lax.Precision.HIGHEST)
    ending = running[:, rows - 1 : rows]
    c_ref[...] = running
    ct_ref[...] = running.T
    logs = jnp.broadcast_to(ending, (heads, 128))
    logs_ref[...] = logs
    fading = jnp.where(live, jnp.exp(ending - running), 0.0)
    k_copy.wait()
    v_copy.wait()
    for h in range(heads):
        kt = k_ref[:, h * width : (h + 1) * width].T.astype(F32)
        scaled = (kt * fading[h : h + 1, :]).astype(BF16)
        states[h] = jnp.dot(scaled, v_ref[:, h * width : (h + 1) * width], preferred_element_type=F32)
    keep = bit(i, 0) * half
    send = half - keep
    for h in range(half):
        kept_ref[h] = states[keep + h]
        msg_ref[h * width : (h + 1) * width, :] = states[send + h].astype(BF16)
    put_logs(msg_ref, half * width, logs)


def up_kernel(level, recv_ref, kept_ref, logs_ref, msg_ref, low_ref, lowlog_ref, next_ref=None, sum_ref=None):
    i = lax.axis_index("seq")
    count, width = kept_ref.shape[0], kept_ref.shape[1]
    upper = bit(i, level) == 1
    own = logs_ref[...]
    other = get_logs(recv_ref, count * width)
    low_logs = jnp.where(upper, other, own)
    lowlog_ref[...] = low_logs
    grown = jnp.exp(jnp.where(upper, own, other))
    start = first_head(i, level)
    which = lax.broadcasted_iota(jnp.int32, grown.shape, 0)
    totals = []
    for h in range(count):
        factor = jnp.sum(jnp.where(which == start + h, grown, 0.0), axis=0, keepdims=True)
        mine = kept_ref[h]
        got = recv_ref[h * width : (h + 1) * width, :].astype(F32)
        low = jnp.where(upper, got, mine)
        high = jnp.where(upper, mine, got)
        low_ref[h] = low
        totals.append(factor * low + high)
    if level > 0:
        for h in range(count):
            msg_ref[h * width : (h + 1) * width, :] = totals[h].astype(BF16)
        if level == 1:
            for h in range(count):
                next_ref[h] = totals[h]
            sum_ref[...] = own + other
            put_logs(msg_ref, count * width, own + other)
        return
    sum_ref[...] = own + other
    half = count // 2
    first = bit(i, 1) == 0
    for h in range(half):
        next_ref[h] = jnp.where(first, totals[h], totals[half + h])
        msg_ref[h * width : (h + 1) * width, :] = jnp.where(first, totals[half + h], totals[h]).astype(BF16)
    put_logs(msg_ref, half * width, own + other)


def middle_kernel(recv_ref, low2_ref, log2_ref, low1_ref, log1_ref, mine_ref, msg_ref):
    i = lax.axis_index("seq")
    count, width = low1_ref.shape[0], low1_ref.shape[1]
    start = first_head(i, 1)
    which = lax.broadcasted_iota(jnp.int32, log1_ref.shape, 0)
    grown2 = jnp.exp(log2_ref[...])
    grown1 = jnp.exp(log1_ref[...])
    upper1 = bit(i, 1) == 1
    upper2 = bit(i, 2) == 1
    for h in range(count):
        factor2 = jnp.sum(jnp.where(which == start + h, grown2, 0.0), axis=0, keepdims=True)
        factor1 = jnp.sum(jnp.where(which == start + h, grown1, 0.0), axis=0, keepdims=True)
        low = recv_ref[h * width : (h + 1) * width, :].astype(F32)
        low = jnp.where(upper2, factor2 * low + low2_ref[h], low)
        high = factor1 * low + low1_ref[h]
        mine_ref[h] = jnp.where(upper1, high, low)
        msg_ref[h * width : (h + 1) * width, :] = jnp.where(upper1, low, high).astype(BF16)


def down_kernel(held_ref, recv_ref, low_ref, lowlog_ref, mine_ref, msg_ref):
    i = lax.axis_index("seq")
    count, width = low_ref.shape[0], low_ref.shape[1]
    half = count // 2
    upper = bit(i, 0) == 1
    grown = jnp.exp(lowlog_ref[...])
    start = first_head(i, 0)
    which = lax.broadcasted_iota(jnp.int32, grown.shape, 0)
    first = bit(i, 1) == 0
    held = [held_ref[h] for h in range(half)]
    got = [recv_ref[h * width : (h + 1) * width, :].astype(F32) for h in range(half)]
    entering = [jnp.where(first, a, b) for a, b in zip(held, got)]
    entering += [jnp.where(first, b, a) for a, b in zip(held, got)]
    for h in range(count):
        factor = jnp.sum(jnp.where(which == start + h, grown, 0.0), axis=0, keepdims=True)
        low = entering[h]
        high = factor * low + low_ref[h]
        mine_ref[h] = jnp.where(upper, high, low)
        msg_ref[h * width : (h + 1) * width, :] = jnp.where(upper, low, high).astype(BF16)


def inside_kernel(bias_ref, q_ref, k_ref, v_ref, c_ref, ct_ref, gain_ref, out_ref, scaled_ref, gain_out_ref):
    gain_out_ref[...] = gain_ref[...]
    i = lax.axis_index("seq")
    rows = q_ref.shape[0]
    heads = c_ref.shape[0]
    width = q_ref.shape[1] // heads
    scale = width ** (-0.5)
    row = lax.broadcasted_iota(jnp.int32, (rows, rows), 0)
    col = lax.broadcasted_iota(jnp.int32, (rows, rows), 1)
    allowed = (col <= row) & (bias_ref[pl.ds(i, 1), :] == 0.0)
    running = c_ref[...]
    running_t = ct_ref[...]
    grown = jnp.exp(running_t) * scale
    for h in range(heads):
        at = slice(h * width, (h + 1) * width)
        scores = lax.dot_general(
            q_ref[:, at], k_ref[:, at], (((1,), (1,)), ((), ())), preferred_element_type=F32
        )
        scaled_ref[:, at] = (q_ref[:, at].astype(F32) * grown[:, h : h + 1]).astype(BF16)
        gaps = running_t[:, h : h + 1] - running[h : h + 1, :]
        weights = jnp.exp(jnp.where(allowed, gaps, NEG))
        intra = (scores * scale * weights).astype(BF16)
        out_ref[:, at] = jnp.dot(intra, v_ref[:, at], preferred_element_type=F32)


def light_kernel(live_ref, q_ref, inside_ref, held_ref, recv_ref, gain_ref, out_ref):
    i = lax.axis_index("seq")
    half, width = held_ref.shape[0], held_ref.shape[1]
    first = bit(i, 0) == 0
    live = live_ref[...] > 0.0
    for h in range(2 * half):
        at = slice(h * width, (h + 1) * width)
        mod = h % half
        held = held_ref[mod].astype(BF16)
        got = recv_ref[mod * width : (mod + 1) * width, :]
        pick_held = first if h < half else jnp.logical_not(first)
        entering = jnp.where(pick_held, held.astype(F32), got.astype(F32)).astype(BF16)
        across = jnp.dot(q_ref[:, at], entering, preferred_element_type=F32)
        combined = inside_ref[:, at] + across
        mean = jnp.mean(combined * combined, axis=-1, keepdims=True)
        normed = combined * lax.rsqrt(mean + 1e-06) * gain_ref[:, at]
        out_ref[:, at] = jnp.where(live, normed, 0.0).astype(BF16)


def unit_columns(rows):
    return jnp.where(lax.broadcasted_iota(jnp.int32, (rows, 128), 1) == 0, 1.0, 0.0).astype(BF16)


def own_kernel(bias_ref, q_ref, k_ref, v_ref, q2_ref, m_ref, l_ref, acc_ref):
    i = lax.axis_index("seq")
    rows, width = k_ref.shape
    heads = q_ref.shape[1] // width
    factor = width ** (-0.5) * LOG2E
    q2_ref[:, width:] = unit_columns(heads * rows)
    for h in range(heads):
        q2_ref[h * rows : (h + 1) * rows, :width] = q_ref[:, h * width : (h + 1) * width]
    row = lax.broadcasted_iota(jnp.int32, (rows, rows), 0)
    col = lax.broadcasted_iota(jnp.int32, (rows, rows), 1)
    allowed = (col <= row) & (bias_ref[pl.ds(i, 1), :] == 0.0)
    scores = jnp.dot(q2_ref[:, :width], k_ref[...].T, preferred_element_type=F32)
    scores = jnp.where(allowed[None], scores.reshape(heads, rows, rows), NEG).reshape(heads * rows, rows)
    peak = jnp.broadcast_to(jnp.max(scores, axis=-1, keepdims=True), (heads * rows, 128))
    probs = [jnp.exp2((scores[:, t : t + 128] - peak) * factor) for t in range(0, rows, 128)]
    m_ref[...] = peak
    l_ref[...] = sum(probs[1:], probs[0])
    acc_ref[...] = jnp.dot(
        jnp.concatenate([p.astype(BF16) for p in probs], axis=1), v_ref[...], preferred_element_type=F32
    )


def attend(q2_ref, blocks, biases, old_ref):
    rows, width = blocks[0].shape[0] // 2, blocks[0].shape[1]
    factor = width ** (-0.5) * LOG2E
    row = lax.broadcasted_iota(jnp.int32, (128, rows), 0)
    biases = [jnp.where(row == 0, bias, 0.0).astype(BF16) for bias in biases]
    keys_t = jnp.concatenate([ref[0:rows, :].T for ref in blocks], axis=1)
    keys_t = jnp.concatenate([keys_t, jnp.concatenate(biases, axis=1)], axis=0)
    values = jnp.concatenate([ref[rows : 2 * rows, :] for ref in blocks], axis=0)
    scores = jnp.dot(q2_ref[...], keys_t, preferred_element_type=F32)
    old = old_ref[...]
    new = jnp.maximum(old, jnp.max(scores, axis=-1, keepdims=True))
    probs = [jnp.exp2((scores[:, t : t + 128] - new) * factor) for t in range(0, scores.shape[1], 128)]
    summed = jnp.dot(
        jnp.concatenate([p.astype(BF16) for p in probs], axis=1), values, preferred_element_type=F32
    )
    return new, jnp.exp2((old - new) * factor), sum(probs[1:], probs[0]), summed


def step_kernel(step, count, blocks, bias_ref, q2_ref, *refs):
    kv_refs, (m_ref, l_ref, acc_ref) = refs[:blocks], refs[-3:]
    i = lax.axis_index("seq")

    @pl.when(i >= step)
    def run():
        wrapped = i + step - count
        biases = [bias_ref[pl.ds(i - step, 1), :]]
        if blocks > 1:
            biases.append(bias_ref[pl.ds(jnp.where(wrapped >= 0, wrapped, count), 1), :])
        new, shrink, total, summed = attend(q2_ref, kv_refs, biases, m_ref)
        m_ref[...] = new
        l_ref[...] = shrink * l_ref[...] + total
        acc_ref[...] = shrink * acc_ref[...] + summed


def last_kernel(step, bias_ref, live_ref, q2_ref, f_ref, m_ref, l_ref, acc_ref, out_ref):
    i = lax.axis_index("seq")
    rows, width = f_ref.shape[0] // 2, f_ref.shape[1]
    heads = q2_ref.shape[0] // rows
    live = live_ref[...] > 0.0

    def finish(total, summed):
        result = summed / jnp.sum(total, axis=-1, keepdims=True)
        for h in range(heads):
            picked = jnp.where(live, result[h * rows : (h + 1) * rows, :], 0.0)
            out_ref[:, h * width : (h + 1) * width] = picked.astype(BF16)

    @pl.when(i >= step)
    def run():
        _, shrink, total, summed = attend(q2_ref, [f_ref], [bias_ref[pl.ds(i - step, 1), :]], m_ref)
        finish(shrink * l_ref[...] + total, shrink * acc_ref[...] + summed)

    @pl.when(i < step)
    def skip():
        finish(l_ref[...], acc_ref[...])


def body(
    light_queries,
    light_keys,
    light_values,
    decay_log,
    norm_gain,
    soft_queries,
    soft_keys,
    soft_values,
    lengths,
):
    rows = light_queries.shape[0]
    heads = decay_log.shape[1]
    width = light_queries.shape[1] // heads
    count = lax.axis_size("seq")
    half = heads // 2
    steps = count // 2
    backs = count - 1 - steps

    def forward(step):
        if step <= backs:
            return [(i, (i + 1) % count) for i in range(count)]
        return [(i, i + 1) for i in range(step - 1, count - 1)]

    backward = [((j + 1) % count, j) for j in range(count)]

    def send(x, pairs):
        return lax.ppermute(x, "seq", pairs)

    def exchange(x, distance):
        return send(x, [(i, i ^ distance) for i in range(count)])

    own_kv = jnp.concatenate([soft_keys, soft_values], axis=0)
    f = send(own_kv, forward(1))
    b = send(own_kv, backward)

    msg, kept, logs, running, running_t, bias, live = call(
        prep_kernel,
        [
            ((half * width + E_ROWS, width), BF16),
            ((half, width, width), F32),
            ((heads, 128), F32),
            ((heads, rows), F32),
            ((rows, heads), F32),
            ((count + 8, rows), F32),
            ((rows, 128), F32),
        ],
        [(False, lengths.reshape(1, count)), (None, pltpu.with_memory_space_constraint(light_keys, pltpu.HBM)), (None, pltpu.with_memory_space_constraint(light_values, pltpu.HBM)), (False, decay_log.T)],
        scratch=[
            pltpu.VMEM((heads, width, width), F32),
            pltpu.VMEM((rows, heads * width), BF16),
            pltpu.VMEM((rows, heads * width), BF16),
            pltpu.SemaphoreType.DMA((2,)),
        ],
        limit=48 * 1024 * 1024,
    )
    saved = []
    n = half
    for level in range(3):
        recv = exchange(msg, 1 << level)
        m = n // 2 if level == 0 else n
        tail = E_ROWS if level < 2 else 0
        onward = [((m, width, width), F32), ((heads, 128), F32)] if level < 2 else []
        msg, low, low_logs, *rest = call(
            partial(up_kernel, level),
            [((m * width + tail, width), BF16), ((n, width, width), F32), ((heads, 128), F32)] + onward,
            [(False, recv), (False, kept), (False, logs)],
        )
        saved.append(((False, low), (False, low_logs)))
        n = m
        if level < 2:
            kept, logs = rest
    recv = send(msg, [(i, (i + 4 if i >= 4 else i - 4) % count) for i in range(count // 2)])
    held, msg = call(
        middle_kernel, [((n, width, width), F32), ((n * width, width), BF16)], [(False, recv), *saved[2], *saved[1]]
    )
    recv = exchange(msg, 2)
    held, msg = call(
        down_kernel,
        [((half, width, width), F32), ((half * width, width), BF16)],
        [(False, held), (False, recv), *saved[0]],
    )
    recv = exchange(msg, 1)
    inside, scaled, gain = call(
        inside_kernel,
        [((rows, heads * width), F32), ((rows, heads * width), BF16), ((1, heads * width), F32)],
        [
            (False, bias),
            (False, light_queries),
            (False, light_keys),
            (False, light_values),
            (False, running),
            (False, running_t),
            (False, norm_gain.reshape(1, heads * width)),
        ],
    )
    (light_out,) = call(
        light_kernel,
        [((rows, heads * width), BF16)],
        [
            (False, live),
            (False, scaled),
            (False, inside),
            (False, held),
            (False, recv),
            (False, gain),
        ],
    )

    soft_rows = soft_queries.shape[1] // width * rows
    stat = ((soft_rows, 128), F32)
    q2, *state = call(
        own_kernel,
        [((soft_rows, width + 128), BF16), stat, stat, stat],
        [(False, bias), (False, soft_queries), (False, soft_keys), (False, soft_values)],
    )
    for step in range(1, steps):
        nf = send(f, forward(step + 1))
        nb = send(b, backward) if step < backs else None
        blocks = [(False, f)] + ([(False, b)] if step <= backs else [])
        at = 2 + len(blocks)
        state = call(
            partial(step_kernel, step, count, len(blocks)),
            [stat, stat, stat],
            [(False, bias), (False, q2)] + blocks + [(False, s) for s in state],
            aliases={at: 0, at + 1: 1, at + 2: 2},
        )
        f, b = nf, nb
    (soft_out,) = call(
        partial(last_kernel, steps),
        [((rows, soft_queries.shape[1]), BF16)],
        [(False, bias), (False, live), (False, q2), (False, f)] + [(False, s) for s in state],
    )
    return (light_out, soft_out)


def solution(mesh):
    return jax.shard_map(
        body,
        mesh=mesh,
        in_specs=(
            P(("groups", "seq"), ("section", "mp")),
            P(("groups", "seq"), ("section", "mp")),
            P(("groups", "seq"), ("section", "mp")),
            P(("groups", "seq"), ("section", "mp")),
            P(("section", "mp")),
            P(("groups", "seq"), ("section", "mp")),
            P(("groups", "seq"), ("section", "mp")),
            P(("groups", "seq"), ("section", "mp")),
            P("groups"),
        ),
        out_specs=(
            P(("groups", "seq"), ("section", "mp")),
            P(("groups", "seq"), ("section", "mp")),
        ),
        check_vma=False,
    )
```

```python
from functools import partial

import jax
import jax.numpy as jnp
from jax import lax
from jax.experimental import pallas as pl
from jax.experimental.pallas import tpu as pltpu
from jax.sharding import PartitionSpec as P


F32 = jnp.float32
BF16 = jnp.bfloat16
NEG = -1e30
LOG2E = 1.4426950408889634
E_ROWS = 32
VMEM = pl.BlockSpec(memory_space=pltpu.VMEM)
ANY = pl.BlockSpec(memory_space=pltpu.HBM)


def call(kernel, out_shape, ins, aliases=None, flops=2_000_000, scratch=(), limit=48 * 1024 * 1024):
    specs = [ANY if s is None else VMEM for s, unused in ins]
    arrays = [a for unused, a in ins]
    outs = [jax.ShapeDtypeStruct(s, d) for s, d in out_shape]
    return pl.pallas_call(
        kernel,
        out_shape=outs,
        in_specs=specs,
        out_specs=[VMEM] * len(outs),
        scratch_shapes=list(scratch),
        input_output_aliases=aliases or {},
        compiler_params=pltpu.CompilerParams(vmem_limit_bytes=limit),
        cost_estimate=pl.CostEstimate(flops=flops, bytes_accessed=1 << 20, transcendentals=0),
    )(*arrays)


def bit(i, level):
    return lax.shift_right_logical(i, level) & 1


def first_head(i, level):
    start = bit(i, 0) * 4
    if level >= 1:
        start += bit(i, 1) * 2
    return start


def put_logs(msg_ref, at, logs):
    hi = logs.astype(BF16)
    rest = logs - hi.astype(F32)
    mid = rest.astype(BF16)
    low = (rest - mid.astype(F32)).astype(BF16)
    both = jnp.concatenate([hi.astype(F32), mid.astype(F32), low.astype(F32), jnp.zeros_like(logs)], axis=0)
    msg_ref[pl.ds(at, E_ROWS), :] = both.astype(BF16)


def get_logs(msg_ref, at):
    rows = msg_ref[pl.ds(at, E_ROWS), :].astype(F32)
    return rows[0:8] + rows[8:16] + rows[16:24]


def prep_kernel(
    len_hbm, k_hbm, v_hbm, dec_hbm, msg_ref, kept_ref, logs_ref, c_ref, ct_ref, bias_ref, live_ref, states, k_ref, v_ref, len_ref, dec_ref, sems
):
    k_copy = pltpu.make_async_copy(k_hbm, k_ref, sems.at[0])
    v_copy = pltpu.make_async_copy(v_hbm, v_ref, sems.at[1])
    len_copy = pltpu.make_async_copy(len_hbm, len_ref, sems.at[2])
    dec_copy = pltpu.make_async_copy(dec_hbm, dec_ref, sems.at[3])
    len_copy.start()
    dec_copy.start()
    k_copy.start()
    v_copy.start()
    i = lax.axis_index("seq")
    rows = k_ref.shape[0]
    heads = dec_ref.shape[0]
    width = k_ref.shape[1] // heads
    half = heads // 2
    blocks = len_ref.shape[1]
    len_copy.wait()
    dec_copy.wait()
    lengths = len_ref[...]
    at = lax.broadcasted_iota(jnp.int32, (1, blocks), 1)
    length = jnp.sum(jnp.where(at == i, lengths, 0), axis=1, keepdims=True)
    live_ref[...] = (lax.broadcasted_iota(jnp.int32, (rows, 128), 0) < length).astype(F32)
    square = (blocks, blocks)
    diagonal = lax.broadcasted_iota(jnp.int32, square, 0) == lax.broadcasted_iota(jnp.int32, square, 1)
    column = jnp.sum(jnp.where(diagonal, lengths, 0), axis=1, keepdims=True)
    dead = lax.broadcasted_iota(jnp.int32, (blocks, rows), 1) >= column
    bias_ref[0:blocks, :] = jnp.where(dead, NEG, 0.0)
    bias_ref[blocks:, :] = jnp.full((8, rows), NEG, F32)
    lane = lax.broadcasted_iota(jnp.int32, (heads, rows), 1)
    live = lane < length
    masked = jnp.where(live, dec_ref[...], 0.0)
    tri = (
        lax.broadcasted_iota(jnp.int32, (rows, rows), 0)
        <= lax.broadcasted_iota(jnp.int32, (rows, rows), 1)
    ).astype(F32)
    running = jnp.dot(masked, tri, preferred_element_type=F32, precision=lax.Precision.HIGHEST)
    ending = running[:, rows - 1 : rows]
    c_ref[...] = running
    ct_ref[...] = running.T
    logs = jnp.broadcast_to(ending, (heads, 128))
    logs_ref[...] = logs
    fading = jnp.where(live, jnp.exp(ending - running), 0.0)
    k_copy.wait()
    v_copy.wait()
    for h in range(heads):
        kt = k_ref[:, h * width : (h + 1) * width].T.astype(F32)
        scaled = (kt * fading[h : h + 1, :]).astype(BF16)
        states[h] = jnp.dot(scaled, v_ref[:, h * width : (h + 1) * width], preferred_element_type=F32)
    keep = bit(i, 0) * half
    send = half - keep
    for h in range(half):
        kept_ref[h] = states[keep + h]
        msg_ref[h * width : (h + 1) * width, :] = states[send + h].astype(BF16)
    put_logs(msg_ref, half * width, logs)


def up_kernel(level, recv_ref, kept_ref, logs_ref, msg_ref, low_ref, lowlog_ref, next_ref=None, sum_ref=None):
    i = lax.axis_index("seq")
    count, width = kept_ref.shape[0], kept_ref.shape[1]
    upper = bit(i, level) == 1
    own = logs_ref[...]
    other = get_logs(recv_ref, count * width)
    low_logs = jnp.where(upper, other, own)
    lowlog_ref[...] = low_logs
    grown = jnp.exp(jnp.where(upper, own, other))
    start = first_head(i, level)
    which = lax.broadcasted_iota(jnp.int32, grown.shape, 0)
    totals = []
    for h in range(count):
        factor = jnp.sum(jnp.where(which == start + h, grown, 0.0), axis=0, keepdims=True)
        mine = kept_ref[h]
        got = recv_ref[h * width : (h + 1) * width, :].astype(F32)
        low = jnp.where(upper, got, mine)
        high = jnp.where(upper, mine, got)
        low_ref[h] = low
        totals.append(factor * low + high)
    if level > 0:
        for h in range(count):
            msg_ref[h * width : (h + 1) * width, :] = totals[h].astype(BF16)
        if level == 1:
            for h in range(count):
                next_ref[h] = totals[h]
            sum_ref[...] = own + other
            put_logs(msg_ref, count * width, own + other)
        return
    sum_ref[...] = own + other
    half = count // 2
    first = bit(i, 1) == 0
    for h in range(half):
        next_ref[h] = jnp.where(first, totals[h], totals[half + h])
        msg_ref[h * width : (h + 1) * width, :] = jnp.where(first, totals[half + h], totals[h]).astype(BF16)
    put_logs(msg_ref, half * width, own + other)


def middle_kernel(recv_ref, low2_ref, log2_ref, low1_ref, log1_ref, mine_ref, msg_ref):
    i = lax.axis_index("seq")
    count, width = low1_ref.shape[0], low1_ref.shape[1]
    start = first_head(i, 1)
    which = lax.broadcasted_iota(jnp.int32, log1_ref.shape, 0)
    grown2 = jnp.exp(log2_ref[...])
    grown1 = jnp.exp(log1_ref[...])
    upper1 = bit(i, 1) == 1
    upper2 = bit(i, 2) == 1
    for h in range(count):
        factor2 = jnp.sum(jnp.where(which == start + h, grown2, 0.0), axis=0, keepdims=True)
        factor1 = jnp.sum(jnp.where(which == start + h, grown1, 0.0), axis=0, keepdims=True)
        low = recv_ref[h * width : (h + 1) * width, :].astype(F32)
        low = jnp.where(upper2, factor2 * low + low2_ref[h], low)
        high = factor1 * low + low1_ref[h]
        mine_ref[h] = jnp.where(upper1, high, low)
        msg_ref[h * width : (h + 1) * width, :] = jnp.where(upper1, low, high).astype(BF16)


def down_kernel(held_ref, recv_ref, low_ref, lowlog_ref, mine_ref, msg_ref):
    i = lax.axis_index("seq")
    count, width = low_ref.shape[0], low_ref.shape[1]
    half = count // 2
    upper = bit(i, 0) == 1
    grown = jnp.exp(lowlog_ref[...])
    start = first_head(i, 0)
    which = lax.broadcasted_iota(jnp.int32, grown.shape, 0)
    first = bit(i, 1) == 0
    held = [held_ref[h] for h in range(half)]
    got = [recv_ref[h * width : (h + 1) * width, :].astype(F32) for h in range(half)]
    entering = [jnp.where(first, a, b) for a, b in zip(held, got)]
    entering += [jnp.where(first, b, a) for a, b in zip(held, got)]
    for h in range(count):
        factor = jnp.sum(jnp.where(which == start + h, grown, 0.0), axis=0, keepdims=True)
        low = entering[h]
        high = factor * low + low_ref[h]
        mine_ref[h] = jnp.where(upper, high, low)
        msg_ref[h * width : (h + 1) * width, :] = jnp.where(upper, low, high).astype(BF16)


def inside_kernel(bias_ref, q_ref, k_ref, v_ref, c_ref, ct_ref, gain_ref, out_ref, scaled_ref, gain_out_ref):
    gain_out_ref[...] = gain_ref[...]
    i = lax.axis_index("seq")
    rows = q_ref.shape[0]
    heads = c_ref.shape[0]
    width = q_ref.shape[1] // heads
    scale = width ** (-0.5)
    row = lax.broadcasted_iota(jnp.int32, (rows, rows), 0)
    col = lax.broadcasted_iota(jnp.int32, (rows, rows), 1)
    allowed = (col <= row) & (bias_ref[pl.ds(i, 1), :] == 0.0)
    running = c_ref[...]
    running_t = ct_ref[...]
    grown = jnp.exp(running_t) * scale
    for h in range(heads):
        at = slice(h * width, (h + 1) * width)
        scores = lax.dot_general(
            q_ref[:, at], k_ref[:, at], (((1,), (1,)), ((), ())), preferred_element_type=F32
        )
        scaled_ref[:, at] = (q_ref[:, at].astype(F32) * grown[:, h : h + 1]).astype(BF16)
        gaps = running_t[:, h : h + 1] - running[h : h + 1, :]
        weights = jnp.exp(jnp.where(allowed, gaps, NEG))
        intra = (scores * scale * weights).astype(BF16)
        out_ref[:, at] = jnp.dot(intra, v_ref[:, at], preferred_element_type=F32)


def light_kernel(live_ref, q_ref, inside_ref, held_ref, recv_ref, gain_ref, out_ref):
    i = lax.axis_index("seq")
    half, width = held_ref.shape[0], held_ref.shape[1]
    first = bit(i, 0) == 0
    live = live_ref[...] > 0.0
    for h in range(2 * half):
        at = slice(h * width, (h + 1) * width)
        mod = h % half
        held = held_ref[mod].astype(BF16)
        got = recv_ref[mod * width : (mod + 1) * width, :]
        pick_held = first if h < half else jnp.logical_not(first)
        entering = jnp.where(pick_held, held.astype(F32), got.astype(F32)).astype(BF16)
        across = jnp.dot(q_ref[:, at], entering, preferred_element_type=F32)
        combined = inside_ref[:, at] + across
        mean = jnp.mean(combined * combined, axis=-1, keepdims=True)
        normed = combined * lax.rsqrt(mean + 1e-06) * gain_ref[:, at]
        out_ref[:, at] = jnp.where(live, normed, 0.0).astype(BF16)


def unit_columns(rows):
    return jnp.where(lax.broadcasted_iota(jnp.int32, (rows, 128), 1) == 0, 1.0, 0.0).astype(BF16)


def own_kernel(bias_ref, q_ref, k_ref, v_ref, q2_ref, m_ref, l_ref, acc_ref):
    i = lax.axis_index("seq")
    rows, width = k_ref.shape
    heads = q_ref.shape[1] // width
    factor = width ** (-0.5) * LOG2E
    q2_ref[:, width:] = unit_columns(heads * rows)
    for h in range(heads):
        q2_ref[h * rows : (h + 1) * rows, :width] = q_ref[:, h * width : (h + 1) * width]
    row = lax.broadcasted_iota(jnp.int32, (rows, rows), 0)
    col = lax.broadcasted_iota(jnp.int32, (rows, rows), 1)
    allowed = (col <= row) & (bias_ref[pl.ds(i, 1), :] == 0.0)
    scores = jnp.dot(q2_ref[:, :width], k_ref[...].T, preferred_element_type=F32)
    scores = jnp.where(allowed[None], scores.reshape(heads, rows, rows), NEG).reshape(heads * rows, rows)
    peak = jnp.broadcast_to(jnp.max(scores, axis=-1, keepdims=True), (heads * rows, 128))
    probs = [jnp.exp2((scores[:, t : t + 128] - peak) * factor) for t in range(0, rows, 128)]
    m_ref[...] = peak
    l_ref[...] = sum(probs[1:], probs[0])
    acc_ref[...] = jnp.dot(
        jnp.concatenate([p.astype(BF16) for p in probs], axis=1), v_ref[...], preferred_element_type=F32
    )


def attend(q2_ref, blocks, biases, old_ref):
    rows, width = blocks[0].shape[0] // 2, blocks[0].shape[1]
    factor = width ** (-0.5) * LOG2E
    row = lax.broadcasted_iota(jnp.int32, (128, rows), 0)
    biases = [jnp.where(row == 0, bias, 0.0).astype(BF16) for bias in biases]
    keys_t = jnp.concatenate([ref[0:rows, :].T for ref in blocks], axis=1)
    keys_t = jnp.concatenate([keys_t, jnp.concatenate(biases, axis=1)], axis=0)
    values = jnp.concatenate([ref[rows : 2 * rows, :] for ref in blocks], axis=0)
    scores = jnp.dot(q2_ref[...], keys_t, preferred_element_type=F32)
    old = old_ref[...]
    new = jnp.maximum(old, jnp.max(scores, axis=-1, keepdims=True))
    probs = [jnp.exp2((scores[:, t : t + 128] - new) * factor) for t in range(0, scores.shape[1], 128)]
    summed = jnp.dot(
        jnp.concatenate([p.astype(BF16) for p in probs], axis=1), values, preferred_element_type=F32
    )
    return new, jnp.exp2((old - new) * factor), sum(probs[1:], probs[0]), summed


def step_kernel(step, count, blocks, bias_ref, q2_ref, *refs):
    kv_refs, (m_ref, l_ref, acc_ref) = refs[:blocks], refs[-3:]
    i = lax.axis_index("seq")

    @pl.when(i >= step)
    def run():
        wrapped = i + step - count
        biases = [bias_ref[pl.ds(i - step, 1), :]]
        if blocks > 1:
            biases.append(bias_ref[pl.ds(jnp.where(wrapped >= 0, wrapped, count), 1), :])
        new, shrink, total, summed = attend(q2_ref, kv_refs, biases, m_ref)
        m_ref[...] = new
        l_ref[...] = shrink * l_ref[...] + total
        acc_ref[...] = shrink * acc_ref[...] + summed


def last_kernel(step, bias_ref, live_ref, q2_ref, f_ref, m_ref, l_ref, acc_ref, out_ref):
    i = lax.axis_index("seq")
    rows, width = f_ref.shape[0] // 2, f_ref.shape[1]
    heads = q2_ref.shape[0] // rows
    live = live_ref[...] > 0.0

    def finish(total, summed):
        result = summed / jnp.sum(total, axis=-1, keepdims=True)
        for h in range(heads):
            picked = jnp.where(live, result[h * rows : (h + 1) * rows, :], 0.0)
            out_ref[:, h * width : (h + 1) * width] = picked.astype(BF16)

    @pl.when(i >= step)
    def run():
        _, shrink, total, summed = attend(q2_ref, [f_ref], [bias_ref[pl.ds(i - step, 1), :]], m_ref)
        finish(shrink * l_ref[...] + total, shrink * acc_ref[...] + summed)

    @pl.when(i < step)
    def skip():
        finish(l_ref[...], acc_ref[...])


def body(
    light_queries,
    light_keys,
    light_values,
    decay_log,
    norm_gain,
    soft_queries,
    soft_keys,
    soft_values,
    lengths,
):
    rows = light_queries.shape[0]
    heads = decay_log.shape[1]
    width = light_queries.shape[1] // heads
    count = lax.axis_size("seq")
    half = heads // 2
    steps = count // 2
    backs = count - 1 - steps

    def forward(step):
        if step <= backs:
            return [(i, (i + 1) % count) for i in range(count)]
        return [(i, i + 1) for i in range(step - 1, count - 1)]

    backward = [((j + 1) % count, j) for j in range(count)]

    def send(x, pairs):
        return lax.ppermute(x, "seq", pairs)

    def exchange(x, distance):
        return send(x, [(i, i ^ distance) for i in range(count)])

    own_kv = jnp.concatenate([soft_keys, soft_values], axis=0)
    f = send(own_kv, forward(1))
    b = send(own_kv, backward)

    msg, kept, logs, running, running_t, bias, live = call(
        prep_kernel,
        [
            ((half * width + E_ROWS, width), BF16),
            ((half, width, width), F32),
            ((heads, 128), F32),
            ((heads, rows), F32),
            ((rows, heads), F32),
            ((count + 8, rows), F32),
            ((rows, 128), F32),
        ],
        [
            (None, pltpu.with_memory_space_constraint(x, pltpu.HBM))
            for x in (lengths.reshape(1, count), light_keys, light_values, decay_log.T)
        ],
        scratch=[
            pltpu.VMEM((heads, width, width), F32),
            pltpu.VMEM((rows, heads * width), BF16),
            pltpu.VMEM((rows, heads * width), BF16),
            pltpu.VMEM((1, count), jnp.int32),
            pltpu.VMEM((heads, rows), F32),
            pltpu.SemaphoreType.DMA((4,)),
        ],
        limit=48 * 1024 * 1024,
    )
    saved = []
    n = half
    for level in range(3):
        recv = exchange(msg, 1 << level)
        m = n // 2 if level == 0 else n
        tail = E_ROWS if level < 2 else 0
        onward = [((m, width, width), F32), ((heads, 128), F32)] if level < 2 else []
        msg, low, low_logs, *rest = call(
            partial(up_kernel, level),
            [((m * width + tail, width), BF16), ((n, width, width), F32), ((heads, 128), F32)] + onward,
            [(False, recv), (False, kept), (False, logs)],
        )
        saved.append(((False, low), (False, low_logs)))
        n = m
        if level < 2:
            kept, logs = rest
    recv = send(msg, [(i, (i + 4 if i >= 4 else i - 4) % count) for i in range(count // 2)])
    held, msg = call(
        middle_kernel, [((n, width, width), F32), ((n * width, width), BF16)], [(False, recv), *saved[2], *saved[1]]
    )
    recv = exchange(msg, 2)
    held, msg = call(
        down_kernel,
        [((half, width, width), F32), ((half * width, width), BF16)],
        [(False, held), (False, recv), *saved[0]],
    )
    recv = exchange(msg, 1)
    inside, scaled, gain = call(
        inside_kernel,
        [((rows, heads * width), F32), ((rows, heads * width), BF16), ((1, heads * width), F32)],
        [
            (False, bias),
            (False, light_queries),
            (False, light_keys),
            (False, light_values),
            (False, running),
            (False, running_t),
            (False, norm_gain.reshape(1, heads * width)),
        ],
    )
    (light_out,) = call(
        light_kernel,
        [((rows, heads * width), BF16)],
        [
            (False, live),
            (False, scaled),
            (False, inside),
            (False, held),
            (False, recv),
            (False, gain),
        ],
    )

    soft_rows = soft_queries.shape[1] // width * rows
    stat = ((soft_rows, 128), F32)
    q2, *state = call(
        own_kernel,
        [((soft_rows, width + 128), BF16), stat, stat, stat],
        [(False, bias), (False, soft_queries), (False, soft_keys), (False, soft_values)],
    )
    for step in range(1, steps):
        nf = send(f, forward(step + 1))
        nb = send(b, backward) if step < backs else None
        blocks = [(False, f)] + ([(False, b)] if step <= backs else [])
        at = 2 + len(blocks)
        state = call(
            partial(step_kernel, step, count, len(blocks)),
            [stat, stat, stat],
            [(False, bias), (False, q2)] + blocks + [(False, s) for s in state],
            aliases={at: 0, at + 1: 1, at + 2: 2},
        )
        f, b = nf, nb
    (soft_out,) = call(
        partial(last_kernel, steps),
        [((rows, soft_queries.shape[1]), BF16)],
        [(False, bias), (False, live), (False, q2), (False, f)] + [(False, s) for s in state],
    )
    return (light_out, soft_out)


def solution(mesh):
    return jax.shard_map(
        body,
        mesh=mesh,
        in_specs=(
            P(("groups", "seq"), ("section", "mp")),
            P(("groups", "seq"), ("section", "mp")),
            P(("groups", "seq"), ("section", "mp")),
            P(("groups", "seq"), ("section", "mp")),
            P(("section", "mp")),
            P(("groups", "seq"), ("section", "mp")),
            P(("groups", "seq"), ("section", "mp")),
            P(("groups", "seq"), ("section", "mp")),
            P("groups"),
        ),
        out_specs=(
            P(("groups", "seq"), ("section", "mp")),
            P(("groups", "seq"), ("section", "mp")),
        ),
        check_vma=False,
    )
```
